32 devices in a mesh: shard: 4 (over x, core), ctx: 2 (over y), tp: 4 (over z).
Axes of the slice: x: 2, y: 2, z: 4, core: 2. Of those that a mesh axis runs over, the one named last changes fastest.
Arguments:
- tokens: bfloat16 [8192, 1024], P(('shard', 'ctx')), may hold values from -6 to 6
- segment_ids: int32 [8192], P('shard'), may hold values from -1 to 3, as said below
- cotangent: bfloat16 [8192, 1024], P(('shard', 'ctx')), may hold values from -6 to 6
- norm_gain: bfloat16 [1024], P('shard'), may hold values from 0.5 to 1.5
- w_query: bfloat16 [1024, 1024], P('shard', 'tp'), may hold values from -0.1875 to 0.1875
- w_key: bfloat16 [1024, 1024], P('shard', 'tp'), may hold values from -0.1875 to 0.1875
- w_value: bfloat16 [1024, 2048], P('shard', 'tp'), may hold values from -0.1875 to 0.1875
- w_outgate: bfloat16 [1024, 2048], P('shard', 'tp'), may hold values from -0.1875 to 0.1875
- w_beta: bfloat16 [1024, 8], P('shard', 'tp'), may hold values from -0.1875 to 0.1875
- w_decay: bfloat16 [1024, 8], P('shard', 'tp'), may hold values from -0.1875 to 0.1875
- decay_bias: bfloat16 [8], P('tp'), may hold values from -8 to -2.5
- conv_query: bfloat16 [4, 8, 128], P(None, 'tp', 'shard'), may hold values from -3 to 3
- conv_key: bfloat16 [4, 8, 128], P(None, 'tp', 'shard'), may hold values from -3 to 3
- conv_value: bfloat16 [4, 8, 256], P(None, 'tp', 'shard'), may hold values from -3 to 3
- out_gain: bfloat16 [8, 256], P('tp', 'shard'), may hold values from 0.5 to 1.5
- w_out: bfloat16 [2048, 1024], P('tp', 'shard'), may hold values from -0.125 to 0.125
- mlp_gain: bfloat16 [1024], P('shard'), may hold values from 0.5 to 1.5
- w_gate: bfloat16 [1024, 2816], P('shard', 'tp'), may hold values from -0.1875 to 0.1875
- w_up: bfloat16 [1024, 2816], P('shard', 'tp'), may hold values from -0.1875 to 0.1875
- w_down: bfloat16 [2816, 1024], P('tp', 'shard'), may hold values from -0.109375 to 0.109375
Outputs:
- output: bfloat16 [8192, 1024], P(('shard', 'ctx'))
- input_grad: float32 [8192, 1024], P(('shard', 'ctx'))
- norm_gain_grad: float32 [1024], P('shard')
- w_query_grad: float32 [1024, 1024], P('shard', 'tp')
- w_key_grad: float32 [1024, 1024], P('shard', 'tp')
- w_value_grad: float32 [1024, 2048], P('shard', 'tp')
- w_outgate_grad: float32 [1024, 2048], P('shard', 'tp')
- w_beta_grad: float32 [1024, 8], P('shard', 'tp')
- w_decay_grad: float32 [1024, 8], P('shard', 'tp')
- decay_bias_grad: float32 [8], P('tp')
- conv_query_grad: float32 [4, 8, 128], P(None, 'tp', 'shard')
- conv_key_grad: float32 [4, 8, 128], P(None, 'tp', 'shard')
- conv_value_grad: float32 [4, 8, 256], P(None, 'tp', 'shard')
- out_gain_grad: float32 [8, 256], P('tp', 'shard')
- w_out_grad: float32 [2048, 1024], P('tp', 'shard')
- mlp_gain_grad: float32 [1024], P('shard')
- w_gate_grad: float32 [1024, 2816], P('shard', 'tp')
- w_up_grad: float32 [1024, 2816], P('shard', 'tp')
- w_down_grad: float32 [2816, 1024], P('tp', 'shard')
The draws below stay inside these ranges and needn't reach their ends.
Inputs may be any that keep to these rules, and one draw needn't show every extreme that they name: `segment_ids`: within each aligned block of 2048 slots (one block a pack), the live slots come first and number between 1280 and 1792; the remaining slots are padding with id -1. Over the live slots ids never fall, and equal ids form one sequence; a pack holds one to four sequences, exactly one of them has 1024 slots, all others fewer, and the last live slot of every pack has id 3.
All inputs are finite; a program needn't handle non-finite values.
Results may differ from the reference program's by a relative error of at most 0.025.
Values may be sent and summed in bfloat16 or wider, within the bound.
A program may use at most 192 MiB of HBM per device.

```python
import jax
import jax.numpy as jnp
from jax import lax

D = 1024
H = 8
DK = 128
DV = 256
FF = 2816
CONV = 4
BLOCK = 64
GT = 2048
TOKENS = 8192
MOST = 1024


def draw_segment_ids(key, part):

    def one_block(block_key):
        live_key, cut_key, start_key = jax.random.split(block_key, 3)
        live_count = jax.random.randint(live_key, (), GT * 5 // 8, GT * 7 // 8 + 1)
        rest_count = live_count - MOST
        cut_point = jax.random.randint(cut_key, (), 1, rest_count)
        long_start = jax.random.randint(start_key, (), 0, rest_count)
        position = jnp.arange(GT, dtype=jnp.int32)
        inside_long = (position >= long_start) & (position < long_start + MOST)
        reduced = jnp.where(position < long_start, position, jnp.where(inside_long, long_start, position - MOST))
        counted = (reduced >= cut_point).astype(jnp.int32)
        labels = counted + (position >= long_start).astype(jnp.int32) + (position >= long_start + MOST).astype(jnp.int32)
        return jnp.where(position < live_count, labels, -1).astype(jnp.int32)
    return jax.vmap(one_block)(jax.random.split(key, TOKENS // GT)).reshape(TOKENS)


def shard_levels(stream_key, shape, shards, smallest, top_value):
    factor_of = 1.0
    for axis_at, blocks in shards:
        heights = jax.random.uniform(jax.random.fold_in(jax.random.fold_in(stream_key, 6), axis_at), (blocks,), jnp.float32, smallest / len(shards), top_value / len(shards))
        factor_of = factor_of * jnp.repeat(jnp.exp(heights), shape[axis_at] // blocks).reshape((-1,) + (1,) * (len(shape) - 1 - axis_at))
    return factor_of


def scatter_about(stream_key, extent, scale, bound, cuts=(), kind=jnp.bfloat16):
    drawn = scale * jax.random.normal(stream_key, extent, jnp.float32)
    if cuts:
        drawn = drawn * shard_levels(stream_key, extent, cuts, -0.22, 0.18)
    return jnp.clip(drawn, -bound, bound).astype(kind)


def setup_inputs(seed: int = 0) -> dict:
    key_list = jax.random.split(jax.random.key(seed), 21)
    tokens = scatter_about(key_list[0], (TOKENS, D), 1.0, 6.0, ((0, 8),))
    segment_ids = draw_segment_ids(jax.random.fold_in(key_list[20], 71), 0)
    cotangent = scatter_about(key_list[2], (TOKENS, D), 1.0, 6.0, ((0, 8),))
    norm_gain = jnp.clip(1.0 + 0.1 * jax.random.normal(key_list[3], (D,), jnp.float32), 0.5, 1.5).astype(jnp.bfloat16)
    w_query = scatter_about(key_list[4], (D, H * DK), D ** -0.5, 0.1875, ((0, 4), (1, 4)))
    w_key = scatter_about(key_list[5], (D, H * DK), D ** -0.5, 0.1875, ((0, 4), (1, 4)))
    w_value = scatter_about(key_list[6], (D, H * DV), D ** -0.5, 0.1875, ((0, 4), (1, 4)))
    w_outgate = scatter_about(key_list[7], (D, H * DV), D ** -0.5, 0.1875, ((0, 4), (1, 4)))
    w_beta = scatter_about(key_list[8], (D, H), D ** -0.5, 0.1875, ((0, 4), (1, 4)))
    w_decay = scatter_about(key_list[9], (D, H), D ** -0.5, 0.1875, ((0, 4), (1, 4)))
    decay_bias = jnp.clip(-8.0 + 5.5 * jax.random.uniform(key_list[10], (H,), jnp.float32) ** shard_levels(key_list[10], (H,), ((0, 4),), -0.2, 0.2), -8.0, -2.5).astype(jnp.bfloat16)
    conv_query = scatter_about(key_list[11], (CONV, H, DK), CONV ** -0.5, 3.0, ((1, 4), (2, 4)))
    conv_key = scatter_about(key_list[12], (CONV, H, DK), CONV ** -0.5, 3.0, ((1, 4), (2, 4)))
    conv_value = scatter_about(key_list[13], (CONV, H, DV), CONV ** -0.5, 3.0, ((1, 4), (2, 4)))
    out_gain = jnp.clip(1.0 + 0.1 * jax.random.normal(key_list[14], (H, DV), jnp.float32), 0.5, 1.5).astype(jnp.bfloat16)
    w_out = scatter_about(key_list[15], (H * DV, D), (H * DV) ** -0.5, 0.125, ((0, 4), (1, 4)))
    mlp_gain = jnp.clip(1.0 + 0.1 * jax.random.normal(key_list[16], (D,), jnp.float32), 0.5, 1.5).astype(jnp.bfloat16)
    w_gate = scatter_about(key_list[17], (D, FF), D ** -0.5, 0.1875, ((0, 4), (1, 4)))
    w_up = scatter_about(key_list[18], (D, FF), D ** -0.5, 0.1875, ((0, 4), (1, 4)))
    w_down = scatter_about(key_list[19], (FF, D), FF ** -0.5, 0.109375, ((0, 4), (1, 4)))
    return {"tokens": tokens, "segment_ids": segment_ids, "cotangent": cotangent, "norm_gain": norm_gain, "w_query": w_query, "w_key": w_key, "w_value": w_value, "w_outgate": w_outgate, "w_beta": w_beta, "w_decay": w_decay, "decay_bias": decay_bias, "conv_query": conv_query, "conv_key": conv_key, "conv_value": conv_value, "out_gain": out_gain, "w_out": w_out, "mlp_gain": mlp_gain, "w_gate": w_gate, "w_up": w_up, "w_down": w_down}


EPSILON = 1e-06

@jax.custom_vjp
def low(v):
    return lax.optimization_barrier(v.astype(jnp.bfloat16)).astype(jnp.float32)

@jax.custom_vjp
def low_back(v):
    return v

def low_keep(v):
    return (low(v), None)

def low_pass(kept, grad):
    return (grad,)

def back_keep(v):
    return (v, None)

def back_low(kept, grad):
    return (low(grad),)
low.defvjp(low_keep, low_pass)
low_back.defvjp(back_keep, back_low)

def matmul(left, right):
    return jnp.dot(left, right, precision=lax.Precision.HIGHEST)

def rms_norm(vector, scale_gain):
    return vector * lax.rsqrt(lax.optimization_barrier(jnp.mean(vector * vector, axis=-1, keepdims=True)) + EPSILON) * scale_gain

def unit_rows(vector):
    return vector * lax.rsqrt(lax.optimization_barrier(jnp.sum(vector * vector, axis=-1, keepdims=True)) + EPSILON)

def short_conv(signal, kernel, segments):
    result = signal * kernel[0]
    for offset in range(1, kernel.shape[0]):
        shifted = jnp.concatenate([jnp.zeros((offset, signal.shape[1]), signal.dtype), signal[:-offset]], axis=0)
        earlier = jnp.concatenate([jnp.full((offset,), -2, jnp.int32), segments[:-offset]], axis=0)
        result = result + jnp.where((earlier == segments)[:, None], shifted, 0.0) * kernel[offset]
    return result

def delta_block(carry_state, pieces):
    query_rows, key_rows, value_rows, beta_rows, decay_rows, seg_rows, before = pieces
    block_span = query_rows.shape[0]
    row_index = lax.broadcasted_iota(jnp.int32, (block_span, block_span), 0)
    col_index = lax.broadcasted_iota(jnp.int32, (block_span, block_span), 1)
    below_diag = row_index >= col_index
    cumulative = jnp.cumsum(decay_rows)
    inside = below_diag & (seg_rows[:, None] == seg_rows[None, :])
    spread = jnp.where(below_diag, cumulative[:, None] - cumulative[None, :], 0.0)
    fading = jnp.where(inside, jnp.exp(spread), 0.0)
    carried = jnp.where(seg_rows == before, jnp.exp(cumulative), 0.0)
    intersection = matmul(key_rows, key_rows.T)
    strict = jnp.where(row_index > col_index, beta_rows[:, None] * fading * intersection, 0.0)
    system = strict + jnp.eye(block_span, dtype=carry_state.dtype)
    target = beta_rows[:, None] * (value_rows - carried[:, None] * matmul(key_rows, carry_state))
    update = jax.scipy.linalg.solve_triangular(system, target, lower=True, unit_diagonal=True)
    scores = fading * matmul(query_rows, key_rows.T)
    output = carried[:, None] * matmul(query_rows, carry_state) + matmul(scores, update)
    next_state = carried[-1] * carry_state + matmul(key_rows.T, fading[-1][:, None] * update)
    return (next_state, output)

def delta_rule(queries, keys_in, values, beta_rows, decay_rows, segments):
    block_count = queries.shape[0] // BLOCK
    before = jnp.concatenate([jnp.full((1,), -2, jnp.int32), segments[:-1]], axis=0)
    before = before.reshape(block_count, BLOCK)[:, 0]
    pieces = (queries.reshape(block_count, BLOCK, -1), keys_in.reshape(block_count, BLOCK, -1), values.reshape(block_count, BLOCK, -1), beta_rows.reshape(block_count, BLOCK), decay_rows.reshape(block_count, BLOCK), segments.reshape(block_count, BLOCK), before)
    start_state = jnp.zeros((queries.shape[1], values.shape[1]), jnp.float32)
    ignored, outputs = lax.scan(jax.checkpoint(delta_block), start_state, pieces)
    return outputs.reshape(queries.shape[0], values.shape[1])

def forward(tokens, norm_gain, w_query, w_key, w_value, w_outgate, w_beta, w_decay, decay_bias, conv_query, conv_key, conv_value, out_gain, w_out, mlp_gain, w_gate, w_up, w_down, segment_ids):
    normed = low(rms_norm(tokens, norm_gain))
    query_raw = low_back(low(matmul(normed, w_query)))
    key_raw = low_back(low(matmul(normed, w_key)))
    value_raw = low_back(low(matmul(normed, w_value)))
    gate_raw = low_back(matmul(normed, w_outgate))
    beta_all = low(jax.nn.sigmoid(matmul(normed, w_beta)))
    decays = low(-jax.nn.softplus(matmul(normed, w_decay) + decay_bias))
    kernel_query = conv_query.reshape(CONV, H * DK)
    kernel_key = conv_key.reshape(CONV, H * DK)
    kernel_value = conv_value.reshape(CONV, H * DV)

    def mix_group(pieces):
        query_rows, key_rows, value_rows, beta_rows, decay_rows, seg_rows = pieces
        queries = unit_rows(jax.nn.silu(short_conv(query_rows, kernel_query, seg_rows)).reshape(GT, H, DK)) * DK ** (-0.5)
        keys_in = unit_rows(jax.nn.silu(short_conv(key_rows, kernel_key, seg_rows)).reshape(GT, H, DK))
        values = jax.nn.silu(short_conv(value_rows, kernel_value, seg_rows)).reshape(GT, H, DV)
        heads_out = jax.vmap(delta_rule, in_axes=(1, 1, 1, 1, 1, None), out_axes=1)(queries, keys_in, values, beta_rows, decay_rows, seg_rows)
        return heads_out.reshape(GT, H * DV)
    groups = TOKENS // GT
    mixed_raw = lax.map(mix_group, (query_raw.reshape(groups, GT, -1), key_raw.reshape(groups, GT, -1), value_raw.reshape(groups, GT, -1), beta_all.reshape(groups, GT, H), decays.reshape(groups, GT, H), segment_ids.reshape(groups, GT)))
    mixed = low_back(low(mixed_raw.reshape(TOKENS, H * DV)))
    per_head = mixed.reshape(TOKENS, H, DV)
    live_rows = (segment_ids >= 0).astype(jnp.float32)[:, None, None]
    gated = rms_norm(per_head, out_gain) * jax.nn.silu(gate_raw).reshape(TOKENS, H, DV) * live_rows
    gated = low(gated.reshape(TOKENS, H * DV))
    attended = low_back(matmul(gated, w_out))
    hidden_in = tokens + attended
    normed_two = low(rms_norm(hidden_in, mlp_gain))
    gate_two = low_back(matmul(normed_two, w_gate))
    up_two = low_back(matmul(normed_two, w_up))
    hidden = low(jax.nn.silu(gate_two) * up_two)
    return hidden_in + matmul(hidden, w_down)

def reference(tokens, segment_ids, cotangent, norm_gain, w_query, w_key, w_value, w_outgate, w_beta, w_decay, decay_bias, conv_query, conv_key, conv_value, out_gain, w_out, mlp_gain, w_gate, w_up, w_down):
    primals = tuple((array_in.astype(jnp.float32) for array_in in (tokens, norm_gain, w_query, w_key, w_value, w_outgate, w_beta, w_decay, decay_bias, conv_query, conv_key, conv_value, out_gain, w_out, mlp_gain, w_gate, w_up, w_down)))

    def wrapped(*params):
        return forward(*params, segment_ids)
    result, pullback = jax.vjp(wrapped, *primals)
    grads = pullback(cotangent.astype(jnp.float32))
    return (result.astype(jnp.bfloat16), grads[0], grads[1], grads[2], grads[3], grads[4], grads[5], grads[6], grads[7], grads[8], grads[9], grads[10], grads[11], grads[12], grads[13], grads[14], grads[15], grads[16], grads[17])
```

```python
import functools
import jax
import jax.numpy as jnp
from jax import lax
from jax.experimental import pallas as pl
from jax.experimental.pallas import tpu as pltpu

F32 = jnp.float32
BF16 = jnp.bfloat16
CHUNK = 128
EPSILON = 1e-06
NN = (((1,), (0,)), ((), ()))
NT = (((1,), (1,)), ((), ()))
TN = (((0,), (0,)), ((), ()))


def mm(left, right, dims=NN):
    return lax.dot_general(
        left.astype(BF16), right.astype(BF16), dims, preferred_element_type=F32
    )


def iotas(size):
    rows = lax.broadcasted_iota(jnp.int32, (size, size), 0)
    cols = lax.broadcasted_iota(jnp.int32, (size, size), 1)
    return rows, cols


def to_row(column, eye):
    return jnp.sum(jnp.where(eye, column, 0.0), axis=0, keepdims=True)


def fades(decay, seg, before):
    size = decay.shape[0]
    rows, cols = iotas(size)
    eye = rows == cols
    decay_row = to_row(decay, eye)
    total_col = jnp.sum(jnp.where(cols <= rows, decay_row, 0.0), axis=1, keepdims=True)
    total_row = jnp.sum(jnp.where(rows <= cols, decay, 0.0), axis=0, keepdims=True)
    inside = (cols <= rows) & (seg == to_row(seg, eye))
    fading = jnp.where(inside, jnp.exp(jnp.minimum(total_col - total_row, 0.0)), 0.0)
    carried = before * jnp.exp(total_col)
    last_col = jnp.where(
        seg == seg[size - 1 :, :], jnp.exp(total_col[size - 1 :, :] - total_col), 0.0
    )
    return fading, carried, last_col


def inverses(lowers):
    size = lowers[0].shape[0]
    rows, cols = iotas(size)
    eye = jnp.where(rows == cols, 1.0, 0.0)
    totals = []
    pair = (rows // 2 == cols // 2) & (rows > cols)
    for lower in lowers:
        totals.append(eye - jnp.where(pair, lower, 0.0))
    half = 2
    while half < size:
        off = (rows // (2 * half) == cols // (2 * half)) & (rows // half > cols // half)
        lows = [t.astype(BF16) for t in totals]
        mids = [mm(jnp.where(off, lower, 0.0), t) for lower, t in zip(lowers, lows)]
        ends = [mm(t, mid) for t, mid in zip(lows, mids)]
        totals = [t - end for t, end in zip(totals, ends)]
        half *= 2
    return totals


def conv_rows(ext_ref, size, taps, masks):
    lines = [ext_ref[8 : 8 + size, :]]
    result = lines[0] * taps[0:1, :]
    for offset in (1, 2, 3):
        shifted = ext_ref[8 - offset : 8 - offset + size, :] * masks[offset - 1]
        result = result + shifted * taps[offset : offset + 1, :]
    return result


def unit_parts(silu, first, size):
    part = silu[:, first : first + size]
    return part, lax.rsqrt(jnp.sum(part * part, axis=1, keepdims=True) + EPSILON)


def prepare_kernel(
    sizes, raw_ref, halo_ref, aux_ref, taps_ref,
    unit_ref, val_ref, inv_ref, wu_ref, mix_ref, just_ref, state_ref, ext_ref,
):
    heads, dk, dv = sizes
    size = raw_ref.shape[0]

    @pl.when(pl.program_id(0) == 0)
    def _():
        ext_ref[0:8, :] = halo_ref[...].astype(F32)
        state_ref[...] = jnp.zeros_like(state_ref)

    @pl.when(pl.program_id(0) > 0)
    def _():
        ext_ref[0:8, :] = ext_ref[size : size + 8, :]

    ext_ref[8 : 8 + size, :] = raw_ref[...].astype(F32)
    aux = aux_ref[...]
    masks = [aux[:, 2 * heads + 2 + m : 2 * heads + 3 + m] for m in range(3)]
    conv = conv_rows(ext_ref, size, taps_ref[...], masks)
    silu = conv * jax.nn.sigmoid(conv)
    seg = aux[:, 2 * heads : 2 * heads + 1]
    before = aux[:, 2 * heads + 1 : 2 * heads + 2]
    rows, cols = iotas(size)
    val_ref[...] = silu[:, 2 * heads * dk :].astype(BF16)
    work = []
    for h in range(heads):
        beta = aux[:, h : h + 1]
        decay = aux[:, heads + h : heads + h + 1]
        q_part, q_norm = unit_parts(silu, h * dk, dk)
        k_part, k_norm = unit_parts(silu, (heads + h) * dk, dk)
        query = q_part * (q_norm * dk ** (-0.5))
        key = k_part * k_norm
        unit_ref[:, h * dk : (h + 1) * dk] = query.astype(BF16)
        unit_ref[:, (heads + h) * dk : (heads + h + 1) * dk] = key.astype(BF16)
        fading, carried, last_col = fades(decay, seg, before)
        both = mm(jnp.concatenate([key, query], axis=0), key, NT)
        just = jnp.where(rows > cols, fading * both[:size], 0.0)
        score = fading * both[size:]
        just_ref[:, h * size : (h + 1) * size] = just.astype(BF16)
        work.append((beta, query, key, carried, last_col, beta * just, score))
    totals = inverses([w[5] for w in work])
    for h, (beta, query, key, carried, last_col, lower, score) in enumerate(work):
        inv = totals[h].astype(BF16)
        inv_ref[:, h * size : (h + 1) * size] = inv
        value = silu[:, 2 * heads * dk + h * dv : 2 * heads * dk + (h + 1) * dv]
        right = jnp.concatenate([(beta * carried) * key, beta * value], axis=1)
        both = mm(inv, right).astype(BF16)
        wu_ref[:, h * (dk + dv) : (h + 1) * (dk + dv)] = both
        faded = jnp.transpose(key * last_col)
        left = jnp.concatenate([score, faded], axis=0).astype(BF16)
        prod = mm(left, both[:, :dk])
        q_eff = carried * query - prod[:size]
        top = jnp.concatenate([q_eff.astype(BF16), left[:size]], axis=1)
        low = jnp.concatenate([(-prod[size:]).astype(BF16), left[size:]], axis=1)
        mix_ref[0, h, 0:size, :] = top
        mix_ref[0, h, size : size + dk, :] = low
        state = state_ref[h]
        deep = jnp.concatenate([state.astype(BF16), both[:, dk:]], axis=0)
        state_ref[h] = carried[size - 1 :, :] * state + mm(low, deep)


def prepare(sizes, raw, halo, aux, taps):
    heads, dk, dv = sizes
    span, width = raw.shape
    blocks = span // CHUNK
    c = CHUNK
    rowed = lambda w: pl.BlockSpec((c, w), lambda i: (i, 0))
    fixed = lambda a: pl.BlockSpec(a.shape, lambda i: (0,) * a.ndim)
    return pl.pallas_call(
        functools.partial(prepare_kernel, sizes),
        grid=(blocks,),
        in_specs=[rowed(width), fixed(halo), rowed(aux.shape[1]), fixed(taps)],
        out_specs=[
            rowed(2 * heads * dk), rowed(heads * dv), rowed(heads * c),
            rowed(heads * (dk + dv)),
            pl.BlockSpec((1, heads, c + dk, c + dk), lambda i: (i, 0, 0, 0)),
            rowed(heads * c),
            pl.BlockSpec((heads, dk, dv), lambda i: (0, 0, 0)),
        ],
        out_shape=[
            jax.ShapeDtypeStruct((span, 2 * heads * dk), BF16),
            jax.ShapeDtypeStruct((span, heads * dv), BF16),
            jax.ShapeDtypeStruct((span, heads * c), BF16),
            jax.ShapeDtypeStruct((span, heads * (dk + dv)), BF16),
            jax.ShapeDtypeStruct((blocks, heads, c + dk, c + dk), BF16),
            jax.ShapeDtypeStruct((span, heads * c), BF16),
            jax.ShapeDtypeStruct((heads, dk, dv), F32),
        ],
        scratch_shapes=[pltpu.VMEM((c + 8, width), F32)],
        name="delta_prepare",
    )(raw, halo, aux, taps)


def apply_kernel(sizes, mix_ref, wu_ref, aux_ref, start_ref, out_ref, states_ref, state_ref):
    heads, dk, dv = sizes
    size = wu_ref.shape[0]

    @pl.when(pl.program_id(0) == 0)
    def _():
        state_ref[...] = start_ref[...]

    aux = aux_ref[...]
    for h in range(heads):
        decay = aux[:, heads + h : heads + h + 1]
        before = aux[size - 1 :, 2 * heads + 1 : 2 * heads + 2]
        through = before * jnp.exp(jnp.sum(decay, axis=0, keepdims=True))
        state = state_ref[h]
        low = state.astype(BF16)
        states_ref[0, h] = low
        first = h * (dk + dv) + dk
        deep = jnp.concatenate([low, wu_ref[:, first : first + dv]], axis=0)
        both = mm(mix_ref[0, h], deep)
        out_ref[:, h * dv : (h + 1) * dv] = both[:size].astype(BF16)
        state_ref[h] = through * state + both[size:]


def apply_states(sizes, mix, wu, aux, start):
    heads, dk, dv = sizes
    span = wu.shape[0]
    blocks = span // CHUNK
    c = CHUNK
    rowed = lambda w: pl.BlockSpec((c, w), lambda i: (i, 0))
    return pl.pallas_call(
        functools.partial(apply_kernel, sizes),
        grid=(blocks,),
        in_specs=[
            pl.BlockSpec((1, heads, c + dk, c + dk), lambda i: (i, 0, 0, 0)),
            rowed(wu.shape[1]), rowed(aux.shape[1]),
            pl.BlockSpec((heads, dk, dv), lambda i: (0, 0, 0)),
        ],
        out_specs=[
            rowed(heads * dv),
            pl.BlockSpec((1, heads, dk, dv), lambda i: (i, 0, 0, 0)),
            pl.BlockSpec((heads, dk, dv), lambda i: (0, 0, 0)),
        ],
        out_shape=[
            jax.ShapeDtypeStruct((span, heads * dv), BF16),
            jax.ShapeDtypeStruct((blocks, heads, dk, dv), BF16),
            jax.ShapeDtypeStruct((heads, dk, dv), F32),
        ],
        name="delta_apply",
    )(mix, wu, aux, start)


def back_chain_kernel(sizes, mix_ref, grad_ref, aux_ref, end_ref, state_ref):
    heads, dk, dv = sizes
    size = grad_ref.shape[0]

    @pl.when(pl.program_id(0) == 0)
    def _():
        state_ref[...] = end_ref[...]

    aux = aux_ref[...]
    for h in range(heads):
        decay = aux[:, heads + h : heads + h + 1]
        before = aux[size - 1 :, 2 * heads + 1 : 2 * heads + 2]
        through = before * jnp.exp(jnp.sum(decay, axis=0, keepdims=True))
        state = state_ref[h]
        deep = jnp.concatenate(
            [grad_ref[:, h * dv : (h + 1) * dv], state.astype(BF16)], axis=0
        )
        state_ref[h] = through * state + mm(mix_ref[0, h, :, 0:dk], deep, TN)


def back_chain(sizes, mix, grad, aux, end):
    heads, dk, dv = sizes
    span = grad.shape[0]
    blocks = span // CHUNK
    c = CHUNK
    last = blocks - 1
    rowed = lambda w: pl.BlockSpec((c, w), lambda i: (last - i, 0))
    return pl.pallas_call(
        functools.partial(back_chain_kernel, sizes),
        grid=(blocks,),
        in_specs=[
            pl.BlockSpec((1, heads, c + dk, c + dk), lambda i: (last - i, 0, 0, 0)),
            rowed(heads * dv), rowed(aux.shape[1]),
            pl.BlockSpec((heads, dk, dv), lambda i: (0, 0, 0)),
        ],
        out_specs=pl.BlockSpec((heads, dk, dv), lambda i: (0, 0, 0)),
        out_shape=jax.ShapeDtypeStruct((heads, dk, dv), F32),
        name="delta_back_chain",
    )(mix, grad, aux, end)


def back_kernel(
    sizes, raw_ref, prev_ref, halo_ref, aux_ref, taps_ref, unit_ref, val_ref, inv_ref, wu_ref,
    mix_ref, just_ref, states_ref, grad_ref, end_ref,
    draw_ref, tail_ref, head_ref, dtaps_ref, daux_ref,
    state_ref, ext_ref, next_ref, zext_ref, dsil_ref,
):
    heads, dk, dv = sizes
    size, width = raw_ref.shape
    step = pl.program_id(0)
    steps = pl.num_programs(0)

    @pl.when(step == 0)
    def _():
        state_ref[...] = end_ref[...]
        next_ref[...] = jnp.zeros_like(next_ref)
        dtaps_ref[...] = jnp.zeros_like(dtaps_ref)

    @pl.when(step == steps - 1)
    def _():
        ext_ref[0:8, :] = halo_ref[...].astype(F32)

    @pl.when(step < steps - 1)
    def _():
        ext_ref[0:8, :] = prev_ref[...].astype(F32)[8:, :]

    x = raw_ref[...].astype(F32)
    ext_ref[8 : 8 + size, :] = x
    aux = aux_ref[...]
    taps = taps_ref[...]
    masks = [aux[:, 2 * heads + 2 + m : 2 * heads + 3 + m] for m in range(3)]
    conv = conv_rows(ext_ref, size, taps, masks)
    sig = jax.nn.sigmoid(conv)
    silu = conv * sig
    seg = aux[:, 2 * heads : 2 * heads + 1]
    before = aux[:, 2 * heads + 1 : 2 * heads + 2]
    rows, cols = iotas(size)
    eye = rows == cols
    lanes = lax.broadcasted_iota(jnp.int32, (size, daux_ref.shape[1]), 1)
    is_last = lax.broadcasted_iota(jnp.int32, (size, 1), 0) == size - 1
    daux = jnp.zeros((size, daux_ref.shape[1]), F32)
    for h in range(heads):
        beta = aux[:, h : h + 1]
        decay = aux[:, heads + h : heads + h + 1]
        fading, carried, last_col = fades(decay, seg, before)
        query = unit_ref[:, h * dk : (h + 1) * dk]
        key = unit_ref[:, (heads + h) * dk : (heads + h + 1) * dk]
        value = val_ref[:, h * dv : (h + 1) * dv]
        inv = inv_ref[:, h * size : (h + 1) * size]
        weight = wu_ref[:, h * (dk + dv) : h * (dk + dv) + dk]
        upper = wu_ref[:, h * (dk + dv) + dk : (h + 1) * (dk + dv)]
        just = just_ref[:, h * size : (h + 1) * size].astype(F32)
        state_in = states_ref[0, h]
        dout = grad_ref[:, h * dv : (h + 1) * dv]
        dend = state_ref[h]
        dend_low = dend.astype(BF16)
        deep = jnp.concatenate([dout, dend_low], axis=0)
        both = mm(mix_ref[0, h], deep, TN)
        through = carried[size - 1 :, :]
        state_ref[h] = through * dend + both[:dk]
        dupd = both[dk:]
        update = (upper.astype(F32) - mm(weight, state_in)).astype(BF16)
        dres = mm(inv, dupd, TN)
        dres_low = dres.astype(BF16)
        left = jnp.concatenate([dout, dres_low], axis=0)
        right = jnp.concatenate([update, state_in], axis=0)
        quad = mm(left, right, NT)
        dscore = quad[:size, :size]
        dq_state = quad[:size, size:]
        dlower = jnp.where(rows > cols, -quad[size:, :size], 0.0)
        dk_state = quad[size:, size:]
        dfaded = mm(update, dend_low, NT)
        dqk = fading * dscore
        dkk = jnp.where(rows > cols, beta * fading, 0.0) * dlower
        query32 = query.astype(F32)
        key32 = key.astype(F32)
        score = mix_ref[0, h, 0:size, dk : dk + size].astype(F32)
        sym = dkk + jnp.transpose(dkk)
        pair = mm(jnp.concatenate([dqk, sym], axis=0), key)
        dquery = carried * dq_state + pair[:size]
        dkey = (
            last_col * dfaded
            + mm(dqk, query, TN)
            - (beta * carried) * dk_state
            + pair[size:]
        )
        kx = jnp.sum(key32 * dk_state, axis=1, keepdims=True)
        dcarried = jnp.sum(query32 * dq_state, axis=1, keepdims=True) - beta * kx
        dcarried = dcarried + jnp.where(
            is_last, jnp.sum(state_in.astype(F32) * dend), 0.0
        )
        dbeta = (
            jnp.sum(dlower * just, axis=1, keepdims=True)
            + jnp.sum(dres * value.astype(F32), axis=1, keepdims=True)
            - carried * kx
        )
        flow = dscore * score + dlower * (beta * just)
        kz = jnp.sum(key32 * dfaded, axis=1, keepdims=True) * last_col
        dtotal = jnp.sum(flow, axis=1, keepdims=True) + dcarried * carried - kz
        dtotal = dtotal + jnp.where(is_last, jnp.sum(kz, axis=0, keepdims=True), 0.0)
        dtotal_row = to_row(dtotal, eye) - jnp.sum(flow, axis=0, keepdims=True)
        ddecay = jnp.sum(jnp.where(cols >= rows, dtotal_row, 0.0), axis=1, keepdims=True)
        daux = daux + jnp.where(lanes == h, dbeta, 0.0)
        daux = daux + jnp.where(lanes == heads + h, ddecay, 0.0)
        dsil_ref[:, 2 * heads * dk + h * dv : 2 * heads * dk + (h + 1) * dv] = beta * dres
        for first, grad, scale in ((h, dquery, dk ** (-0.5)), (heads + h, dkey, 1.0)):
            part, norm = unit_parts(silu, first * dk, dk)
            unit = part * norm
            grad = grad * scale
            inner = jnp.sum(unit * grad, axis=1, keepdims=True)
            dsil_ref[:, first * dk : (first + 1) * dk] = norm * (grad - unit * inner)
    daux_ref[...] = daux
    dconv = dsil_ref[...] * (sig * (1.0 + conv * (1.0 - sig)))
    draw = dconv * taps[0:1, :]
    dtaps_ref[0:1, :] += jnp.sum(dconv * x, axis=0, keepdims=True)
    halo = halo_ref[...].astype(F32)
    head = jnp.zeros((8, width), F32)
    for m in (1, 2, 3):
        moved = dconv * masks[m - 1]
        zext_ref[8 : 8 + size, :] = moved
        zext_ref[8 + size :, :] = next_ref[m - 1]
        next_ref[m - 1] = moved[0:8, :]
        shifted = zext_ref[8 + m : 8 + m + size, :]
        draw = draw + shifted * taps[m : m + 1, :]
        dtaps_ref[m : m + 1, :] += jnp.sum(shifted * x, axis=0, keepdims=True)

        @pl.when(step == steps - 1)
        def _():
            zext_ref[0:8, :] = jnp.zeros((8, width), F32)
            edge = zext_ref[m : m + 8, :]
            dtaps_ref[m : m + 1, :] += jnp.sum(edge * halo, axis=0, keepdims=True)
            grown = edge * taps[m : m + 1, :]
            if m == 1:
                head_ref[...] = grown
            else:
                head_ref[...] += grown

    draw_ref[...] = draw.astype(BF16)

    @pl.when(step == 0)
    def _():
        tail_ref[...] = draw[size - 8 :, :]


def back_states(sizes, raw, halo, aux, taps, unit, val, inv, wu, mix, just, states, grad, end):
    heads, dk, dv = sizes
    span, width = raw.shape
    blocks = span // CHUNK
    c = CHUNK
    last = blocks - 1
    rowed = lambda w: pl.BlockSpec((c, w), lambda i: (last - i, 0))
    fixed = lambda shape: pl.BlockSpec(shape, lambda i: (0,) * len(shape))
    per16 = c // 16
    prev = pl.BlockSpec((16, width), lambda i: (jnp.maximum((last - i) * per16 - 1, 0), 0))
    return pl.pallas_call(
        functools.partial(back_kernel, sizes),
        grid=(blocks,),
        in_specs=[
            rowed(width), prev, fixed(halo.shape), rowed(aux.shape[1]), fixed(taps.shape),
            rowed(unit.shape[1]), rowed(val.shape[1]), rowed(inv.shape[1]), rowed(wu.shape[1]),
            pl.BlockSpec((1, heads, c + dk, c + dk), lambda i: (last - i, 0, 0, 0)),
            rowed(just.shape[1]),
            pl.BlockSpec((1, heads, dk, dv), lambda i: (last - i, 0, 0, 0)),
            rowed(heads * dv), fixed(end.shape),
        ],
        out_specs=[
            rowed(width), fixed((8, width)), fixed((8, width)), fixed((8, width)), rowed(8),
        ],
        out_shape=[
            jax.ShapeDtypeStruct((span, width), BF16),
            jax.ShapeDtypeStruct((8, width), F32),
            jax.ShapeDtypeStruct((8, width), F32),
            jax.ShapeDtypeStruct((8, width), F32),
            jax.ShapeDtypeStruct((span, 8), F32),
        ],
        scratch_shapes=[
            pltpu.VMEM((heads, dk, dv), F32),
            pltpu.VMEM((c + 8, width), F32),
            pltpu.VMEM((3, 8, width), F32),
            pltpu.VMEM((c + 16, width), F32),
            pltpu.VMEM((c, width), F32),
        ],
        name="delta_back",
    )(raw, raw, halo, aux, taps, unit, val, inv, wu, mix, just, states, grad, end)


from jax.sharding import PartitionSpec as P


def dot_plain(left, right):
    return jnp.dot(left, right, preferred_element_type=F32)


def dot_back(left, right):
    return lax.dot_general(left, right, NT, preferred_element_type=F32)


def dot_outer(left, right):
    return lax.dot_general(left, right, TN, preferred_element_type=F32)


def rms_norm(vector, scale_gain):
    return (
        vector * lax.rsqrt(jnp.mean(vector * vector, axis=-1, keepdims=True) + EPSILON) * scale_gain
    )


def gated_norm(mixed_in, gate_in, gain_in, live_rows):
    head_count = gain_in.shape[0]
    per_head = mixed_in.reshape(mixed_in.shape[0], head_count, -1)
    gated_rows = rms_norm(per_head, gain_in) * jax.nn.silu(gate_in).reshape(per_head.shape)
    return (gated_rows * live_rows[:, None, None]).reshape(mixed_in.shape)


def gate_rates(beta_lin, decay_lin, bias_in):
    return (jax.nn.sigmoid(beta_lin), -jax.nn.softplus(decay_lin + bias_in))


def row_facts(segment_ids, first, span):
    def at(offset):
        moved = segment_ids
        if offset:
            moved = jnp.concatenate(
                [jnp.full((offset,), -2, jnp.int32), segment_ids[:-offset]], axis=0
            )
        return lax.dynamic_slice_in_dim(moved, first, span)

    here = at(0)
    before = jnp.repeat(at(1).reshape(-1, CHUNK)[:, 0], CHUNK)
    flags = [here == before] + [here == at(m) for m in (1, 2, 3)]
    return here, [here.astype(F32)] + [f.astype(F32) for f in flags]


def scatter_sum(parts, axis):
    low = parts.astype(BF16)
    out = lax.psum_scatter(low, "shard", scatter_dimension=axis, tiled=True)
    return lax.psum(out, "ctx").astype(F32)


def shards(
    tokens, segment_ids, cotangent, norm_gain, w_query, w_key, w_value, w_outgate, w_beta, w_decay,
    decay_bias, conv_query, conv_key, conv_value, out_gain, w_out, mlp_gain, w_gate, w_up, w_down,
):
    ctx_size = lax.axis_size("ctx")
    ctx_rank = lax.axis_index("ctx")
    shard_size = lax.axis_size("shard")
    rows_here, model = tokens.shape
    heads = decay_bias.shape[0]
    dk = conv_query.shape[2] * shard_size
    dv = conv_value.shape[2] * shard_size
    sizes = (heads, dk, dv)
    gather = lambda v, axis: lax.all_gather(v, "shard", axis=axis, tiled=True)
    mixer_w = gather(jnp.concatenate([w_query, w_key, w_value, w_outgate], axis=1), 0)
    mlp_w = gather(jnp.concatenate([w_gate, w_up], axis=1), 0)
    out_w = gather(w_out, 1)
    down_w = gather(w_down, 1)
    tiny = [norm_gain, mlp_gain, w_beta, w_decay, conv_query, conv_key, conv_value, out_gain]
    flat = jnp.concatenate([v.reshape(-1) for v in tiny])
    flat = lax.all_gather(flat, "shard", axis=0)
    cuts, at = [], 0
    for v in tiny:
        cuts.append(flat[:, at : at + v.size].reshape((shard_size,) + v.shape))
        at += v.size
    gain_one = cuts[0].reshape(-1).astype(F32)
    gain_two = cuts[1].reshape(-1).astype(F32)
    small_w = jnp.concatenate([cuts[2], cuts[3]], axis=2).reshape(model, 2 * heads)
    taps = [jnp.moveaxis(c, 0, 2).reshape(c.shape[1], -1) for c in cuts[4:7]]
    taps = jnp.concatenate(taps, axis=1).astype(F32)
    head_gain = jnp.moveaxis(cuts[7], 0, 1).reshape(heads, dv).astype(F32)
    conv_width = taps.shape[1]

    here, facts = row_facts(segment_ids, ctx_rank * rows_here, rows_here)
    live_rows = (here >= 0).astype(F32)
    inputs32 = tokens.astype(F32)
    normed32, norm_one_back = jax.vjp(rms_norm, inputs32, gain_one)
    normed = normed32.astype(BF16)
    raw = dot_plain(normed, mixer_w[:, :conv_width]).astype(BF16)
    gate_raw = dot_plain(normed, mixer_w[:, conv_width:])
    small_lin = dot_plain(normed, small_w)
    (beta_rows, decays), rates_back = jax.vjp(
        gate_rates, small_lin[:, :heads], small_lin[:, heads:], decay_bias.astype(F32)
    )
    low = lambda v: v.astype(BF16).astype(F32)
    columns = [low(beta_rows)[:, h] for h in range(heads)]
    columns += [low(decays)[:, h] for h in range(heads)] + facts
    columns += [jnp.zeros((rows_here,), F32)] * (16 - len(columns))
    aux = jnp.stack(columns, axis=1)
    ahead = [(i, i + 1) for i in range(ctx_size - 1)]
    behind = [(i + 1, i) for i in range(ctx_size - 1)]
    halo = lax.ppermute(raw[rows_here - 8 :], "ctx", ahead)
    unit, val, inv, wu, mix, just, total = prepare(sizes, raw, halo, aux, taps)
    start = lax.ppermute(total, "ctx", ahead)
    for _ in range(ctx_size - 2):
        start = lax.ppermute(apply_states(sizes, mix, wu, aux, start)[2], "ctx", ahead)
    mixed, states, _ = apply_states(sizes, mix, wu, aux, start)

    gated32, gated_back = jax.vjp(
        lambda mixed_in, gate_in, gain_in: gated_norm(mixed_in, gate_in, gain_in, live_rows),
        mixed.astype(F32), gate_raw, head_gain,
    )
    gated_rows = gated32.astype(BF16)
    attended = lax.psum(dot_plain(gated_rows, out_w).astype(BF16), "tp").astype(F32)
    hidden_in = inputs32 + attended
    normed_two32, norm_two_back = jax.vjp(rms_norm, hidden_in, gain_two)
    normed_two = normed_two32.astype(BF16)
    both_two = dot_plain(normed_two, mlp_w)
    units = w_gate.shape[1]
    gate_two, up_two = both_two[:, :units], both_two[:, units:]
    sigmoid_two = jax.nn.sigmoid(gate_two)
    activated = gate_two * sigmoid_two
    hidden = (activated * up_two).astype(BF16)
    mlp_out = lax.psum(dot_plain(hidden, down_w).astype(BF16), "tp").astype(F32)
    result = (hidden_in + mlp_out).astype(BF16)
    grad_hidden = dot_back(cotangent, down_w)
    gate_slope = sigmoid_two * (1.0 + gate_two * (1.0 - sigmoid_two))
    grad_gate = (grad_hidden * up_two * gate_slope).astype(BF16)
    grad_up = (grad_hidden * activated).astype(BF16)
    grad_both = jnp.concatenate([grad_gate, grad_up], axis=1)
    part_mlp = scatter_sum(dot_outer(normed_two, grad_both), 0)
    part_down = scatter_sum(dot_outer(hidden, cotangent), 1)
    grad_normed_two = lax.psum(dot_back(grad_both, mlp_w).astype(BF16), "tp").astype(F32)
    grad_hidden_in, grad_gain_two = norm_two_back(grad_normed_two)
    grad_hidden_in = grad_hidden_in + cotangent.astype(F32)
    grad_branch = grad_hidden_in.astype(BF16)
    part_out = scatter_sum(dot_outer(gated_rows, grad_branch), 1)
    grad_gated = dot_back(grad_branch, out_w)
    grad_mixed, grad_gate_raw, grad_head_gain = gated_back(grad_gated)
    grad_mixed = grad_mixed.astype(BF16)
    zero = jnp.zeros((heads, dk, dv), F32)
    end = lax.ppermute(back_chain(sizes, mix, grad_mixed, aux, zero), "ctx", behind)
    for _ in range(ctx_size - 2):
        end = lax.ppermute(back_chain(sizes, mix, grad_mixed, aux, end), "ctx", behind)
    draw, tail, head, dtaps, daux = back_states(
        sizes, raw, halo, aux, taps, unit, val, inv, wu, mix, just, states, grad_mixed, end
    )
    tail = (tail + lax.ppermute(head, "ctx", behind)).astype(BF16)
    draw = lax.dynamic_update_slice(draw, tail, (rows_here - 8, 0))
    grad_gate_low = grad_gate_raw.astype(BF16)
    grad_beta_lin, grad_decay_lin, grad_bias = rates_back(
        (daux[:, :heads], daux[:, heads : 2 * heads])
    )
    grad_small = jnp.concatenate([grad_beta_lin, grad_decay_lin], axis=1).astype(BF16)
    grad_mix = jnp.concatenate([draw, grad_gate_low], axis=1)
    grad_mixer_w = dot_outer(normed, grad_mix)
    grad_small_w = dot_outer(normed, grad_small)
    grad_normed_part = dot_back(grad_mix, mixer_w) + dot_back(grad_small, small_w)
    grad_normed = lax.psum(grad_normed_part.astype(BF16), "tp").astype(F32)
    grad_inputs, grad_gain_one = norm_one_back(grad_normed)
    input_grad = grad_inputs + grad_hidden_in
    part_mixer = scatter_sum(grad_mixer_w, 0)
    split = lambda v: v.reshape(shard_size, -1)
    taps_parts = []
    first = 0
    for width in (heads * dk, heads * dk, heads * dv):
        part = dtaps[:4, first : first + width].reshape(4, heads, shard_size, -1)
        taps_parts.append(jnp.moveaxis(part, 2, 0))
        first += width
    tiny_grads = [
        split(grad_gain_one), split(grad_gain_two), split(grad_small_w),
        split(jnp.broadcast_to(grad_bias[None], (shard_size, heads))),
        *[split(p) for p in taps_parts],
        split(jnp.moveaxis(grad_head_gain.reshape(heads, shard_size, -1), 1, 0)),
    ]
    shapes = [
        norm_gain.shape, mlp_gain.shape, (w_beta.shape[0], 2 * heads), decay_bias.shape,
        conv_query.shape, conv_key.shape, conv_value.shape, out_gain.shape,
    ]
    packed = jnp.concatenate(tiny_grads, axis=1)
    packed = lax.psum(packed, ("shard", "ctx"))
    mine = lax.dynamic_slice_in_dim(packed, lax.axis_index("shard"), 1, 0)[0]
    small, at = [], 0
    for shape in shapes:
        count = 1
        for n in shape:
            count *= n
        small.append(mine[at : at + count].reshape(shape))
        at += count
    qw, vw = heads * dk, heads * dv
    return (
        result,
        input_grad,
        small[0],
        part_mixer[:, :qw],
        part_mixer[:, qw : 2 * qw],
        part_mixer[:, 2 * qw : 2 * qw + vw],
        part_mixer[:, 2 * qw + vw :],
        small[2][:, :heads],
        small[2][:, heads:],
        small[3],
        small[4],
        small[5],
        small[6],
        small[7],
        part_out,
        small[1],
        part_mlp[:, :units],
        part_mlp[:, units:],
        part_down,
    )


def solution(mesh):
    rows = P(("shard", "ctx"), None)
    cols = P("shard", "tp")
    taps = P(None, "tp", "shard")
    turned = P("tp", "shard")
    in_specs = (
        rows, P("shard"), rows, P("shard"), cols, cols, cols, cols, cols, cols, P("tp"),
        taps, taps, taps, turned, turned, P("shard"), cols, cols, turned,
    )
    out_specs = (
        rows, rows, P("shard"), cols, cols, cols, cols, cols, cols, P("tp"),
        taps, taps, taps, turned, turned, P("shard"), cols, cols, turned,
    )
    return jax.shard_map(shards, mesh=mesh, in_specs=in_specs, out_specs=out_specs, check_vma=False)
```

```python
import functools
import jax
import jax.numpy as jnp
from jax import lax
from jax.experimental import pallas as pl
from jax.experimental.pallas import tpu as pltpu
from jax.sharding import PartitionSpec as P

F32 = jnp.float32
BF16 = jnp.bfloat16
CHUNK = 128
EPSILON = 1e-06
NN = (((1,), (0,)), ((), ()))
NT = (((1,), (1,)), ((), ()))
TN = (((0,), (0,)), ((), ()))


def mm(left, right, dims=NN):
    return lax.dot_general(
        left.astype(BF16), right.astype(BF16), dims, preferred_element_type=F32
    )


def iotas(size):
    rows = lax.broadcasted_iota(jnp.int32, (size, size), 0)
    cols = lax.broadcasted_iota(jnp.int32, (size, size), 1)
    return rows, cols


def to_row(column, eye):
    return jnp.sum(jnp.where(eye, column, 0.0), axis=0, keepdims=True)


def fades(decay, seg, before):
    size = decay.shape[0]
    rows, cols = iotas(size)
    eye = rows == cols
    decay_row = to_row(decay, eye)
    total_col = jnp.sum(jnp.where(cols <= rows, decay_row, 0.0), axis=1, keepdims=True)
    total_row = jnp.sum(jnp.where(rows <= cols, decay, 0.0), axis=0, keepdims=True)
    inside = (cols <= rows) & (seg == to_row(seg, eye))
    fading = jnp.where(inside, jnp.exp(jnp.minimum(total_col - total_row, 0.0)), 0.0)
    carried = before * jnp.exp(total_col)
    last_col = jnp.where(
        seg == seg[size - 1 :, :], jnp.exp(total_col[size - 1 :, :] - total_col), 0.0
    )
    return fading, carried, last_col


def inverses(lowers):
    size = lowers[0].shape[0]
    rows, cols = iotas(size)
    eye = jnp.where(rows == cols, 1.0, 0.0)
    totals = []
    pair = (rows // 2 == cols // 2) & (rows > cols)
    for lower in lowers:
        totals.append(eye - jnp.where(pair, lower, 0.0))
    half = 2
    while half < size:
        off = (rows // (2 * half) == cols // (2 * half)) & (rows // half > cols // half)
        lows = [t.astype(BF16) for t in totals]
        mids = [mm(jnp.where(off, lower, 0.0), t) for lower, t in zip(lowers, lows)]
        ends = [mm(t, mid) for t, mid in zip(lows, mids)]
        totals = [t - end for t, end in zip(totals, ends)]
        half *= 2
    return totals


def conv_rows(ext_ref, size, taps, masks):
    lines = [ext_ref[8 : 8 + size, :]]
    result = lines[0] * taps[0:1, :]
    for offset in (1, 2, 3):
        shifted = ext_ref[8 - offset : 8 - offset + size, :] * masks[offset - 1]
        result = result + shifted * taps[offset : offset + 1, :]
    return result


def unit_parts(silu, first, size):
    part = silu[:, first : first + size]
    return part, lax.rsqrt(jnp.sum(part * part, axis=1, keepdims=True) + EPSILON)


AUX = 16
FACTS = 5


def rates(heads, lin, facts):
    lane = lax.broadcasted_iota(jnp.int32, lin.shape, 1)
    sig = jax.nn.sigmoid(lin)
    soft = jnp.maximum(lin, 0.0) + jnp.log1p(jnp.exp(-jnp.abs(lin)))
    main = jnp.where(lane < heads, sig, -soft).astype(BF16).astype(F32)[:, : 2 * heads]
    slope = jnp.where(lane < heads, sig * (1.0 - sig), -sig)[:, : 2 * heads]
    rest = AUX - 4 * heads - facts.shape[1]
    pad = jnp.zeros((lin.shape[0], rest), F32)
    return jnp.concatenate([main, facts, slope, pad], axis=1)


def prepare_kernel(
    sizes, raw_ref, halo_ref, lin_ref, bias_ref, facts_ref, taps_ref,
    unit_ref, val_ref, inv_ref, wu_ref, mix_ref, just_ref, state_ref, aux_ref, ext_ref,
):
    heads, dk, dv = sizes
    size = raw_ref.shape[0]
    aux_ref[...] = rates(heads, lin_ref[...] + bias_ref[...], facts_ref[...])

    @pl.when(pl.program_id(0) == 0)
    def _():
        ext_ref[0:8, :] = halo_ref[...].astype(F32)
        state_ref[...] = jnp.zeros_like(state_ref)

    @pl.when(pl.program_id(0) > 0)
    def _():
        ext_ref[0:8, :] = ext_ref[size : size + 8, :]

    ext_ref[8 : 8 + size, :] = raw_ref[...].astype(F32)
    aux = aux_ref[...]
    masks = [aux[:, 2 * heads + 2 + m : 2 * heads + 3 + m] for m in range(3)]
    conv = conv_rows(ext_ref, size, taps_ref[...], masks)
    silu = conv * jax.nn.sigmoid(conv)
    seg = aux[:, 2 * heads : 2 * heads + 1]
    before = aux[:, 2 * heads + 1 : 2 * heads + 2]
    rows, cols = iotas(size)
    val_ref[...] = silu[:, 2 * heads * dk :].astype(BF16)
    work = []
    for h in range(heads):
        beta = aux[:, h : h + 1]
        decay = aux[:, heads + h : heads + h + 1]
        q_part, q_norm = unit_parts(silu, h * dk, dk)
        k_part, k_norm = unit_parts(silu, (heads + h) * dk, dk)
        query = q_part * (q_norm * dk ** (-0.5))
        key = k_part * k_norm
        unit_ref[:, h * dk : (h + 1) * dk] = query.astype(BF16)
        unit_ref[:, (heads + h) * dk : (heads + h + 1) * dk] = key.astype(BF16)
        fading, carried, last_col = fades(decay, seg, before)
        both = mm(jnp.concatenate([key, query], axis=0), key, NT)
        just = jnp.where(rows > cols, fading * both[:size], 0.0)
        score = fading * both[size:]
        just_ref[:, h * size : (h + 1) * size] = just.astype(BF16)
        work.append((beta, query, key, carried, last_col, beta * just, score))
    totals = inverses([w[5] for w in work])
    for h, (beta, query, key, carried, last_col, lower, score) in enumerate(work):
        inv = totals[h].astype(BF16)
        inv_ref[:, h * size : (h + 1) * size] = inv
        value = silu[:, 2 * heads * dk + h * dv : 2 * heads * dk + (h + 1) * dv]
        right = jnp.concatenate([(beta * carried) * key, beta * value], axis=1)
        both = mm(inv, right).astype(BF16)
        wu_ref[:, h * (dk + dv) : (h + 1) * (dk + dv)] = both
        faded = jnp.transpose(key * last_col)
        left = jnp.concatenate([score, faded], axis=0).astype(BF16)
        prod = mm(left, both[:, :dk])
        q_eff = carried * query - prod[:size]
        top = jnp.concatenate([q_eff.astype(BF16), left[:size]], axis=1)
        low = jnp.concatenate([(-prod[size:]).astype(BF16), left[size:]], axis=1)
        mix_ref[0, h, 0:size, :] = top
        mix_ref[0, h, size : size + dk, :] = low
        state = state_ref[h]
        deep = jnp.concatenate([state.astype(BF16), both[:, dk:]], axis=0)
        state_ref[h] = carried[size - 1 :, :] * state + mm(low, deep)


def prepare(sizes, raw, halo, gates, bias, facts, taps):
    heads, dk, dv = sizes
    span, width = raw.shape
    blocks = span // CHUNK
    c = CHUNK
    rowed = lambda w: pl.BlockSpec((c, w), lambda i: (i, 0))
    fixed = lambda a: pl.BlockSpec(a.shape, lambda i: (0,) * a.ndim)
    return pl.pallas_call(
        functools.partial(prepare_kernel, sizes),
        grid=(blocks,),
        in_specs=[
            rowed(width), fixed(halo), pl.BlockSpec((c, 128), lambda i: (i, heads * dv // 128)),
            fixed(bias), rowed(facts.shape[1]), fixed(taps),
        ],
        out_specs=[
            rowed(2 * heads * dk), rowed(heads * dv), rowed(heads * c),
            rowed(heads * (dk + dv)),
            pl.BlockSpec((1, heads, c + dk, c + dk), lambda i: (i, 0, 0, 0)),
            rowed(heads * c),
            pl.BlockSpec((heads, dk, dv), lambda i: (0, 0, 0)),
            rowed(AUX),
        ],
        out_shape=[
            jax.ShapeDtypeStruct((span, 2 * heads * dk), BF16),
            jax.ShapeDtypeStruct((span, heads * dv), BF16),
            jax.ShapeDtypeStruct((span, heads * c), BF16),
            jax.ShapeDtypeStruct((span, heads * (dk + dv)), BF16),
            jax.ShapeDtypeStruct((blocks, heads, c + dk, c + dk), BF16),
            jax.ShapeDtypeStruct((span, heads * c), BF16),
            jax.ShapeDtypeStruct((heads, dk, dv), F32),
            jax.ShapeDtypeStruct((span, AUX), F32),
        ],
        scratch_shapes=[pltpu.VMEM((c + 8, width), F32)],
        name="delta_prepare",
    )(raw, halo, gates, bias, facts, taps)


def through_of(heads, aux, h):
    decay = aux[:, heads + h : heads + h + 1]
    before = aux[aux.shape[0] - 1 :, 2 * heads + 1 : 2 * heads + 2]
    return before * jnp.exp(jnp.sum(decay, axis=0, keepdims=True))


def apply_step(sizes, aux, mix_ref, wu_ref, states_ref, state_ref):
    heads, dk, dv = sizes
    size = wu_ref.shape[0]
    outs = []
    for h in range(heads):
        state = state_ref[h]
        low = state.astype(BF16)
        states_ref[0, h] = low
        first = h * (dk + dv) + dk
        deep = jnp.concatenate([low, wu_ref[:, first : first + dv]], axis=0)
        both = mm(mix_ref[0, h], deep)
        outs.append(both[:size].astype(BF16))
        state_ref[h] = through_of(heads, aux, h) * state + both[size:]
    return outs


def apply_kernel(sizes, mix_ref, wu_ref, aux_ref, start_ref, out_ref, states_ref, state_ref):
    @pl.when(pl.program_id(0) == 0)
    def _():
        state_ref[...] = start_ref[...]

    dv = sizes[2]
    outs = apply_step(sizes, aux_ref[...], mix_ref, wu_ref, states_ref, state_ref)
    for h, out in enumerate(outs):
        out_ref[:, h * dv : (h + 1) * dv] = out


def apply_states(sizes, mix, wu, aux, start):
    heads, dk, dv = sizes
    span = wu.shape[0]
    blocks = span // CHUNK
    c = CHUNK
    rowed = lambda w: pl.BlockSpec((c, w), lambda i: (i, 0))
    return pl.pallas_call(
        functools.partial(apply_kernel, sizes),
        grid=(blocks,),
        in_specs=[
            pl.BlockSpec((1, heads, c + dk, c + dk), lambda i: (i, 0, 0, 0)),
            rowed(wu.shape[1]), rowed(aux.shape[1]),
            pl.BlockSpec((heads, dk, dv), lambda i: (0, 0, 0)),
        ],
        out_specs=[
            rowed(heads * dv),
            pl.BlockSpec((1, heads, dk, dv), lambda i: (i, 0, 0, 0)),
            pl.BlockSpec((heads, dk, dv), lambda i: (0, 0, 0)),
        ],
        out_shape=[
            jax.ShapeDtypeStruct((span, heads * dv), BF16),
            jax.ShapeDtypeStruct((blocks, heads, dk, dv), BF16),
            jax.ShapeDtypeStruct((heads, dk, dv), F32),
        ],
        name="delta_apply",
    )(mix, wu, aux, start)


def back_chain_step(sizes, aux, mix_ref, grads, state_ref):
    heads, dk, _ = sizes
    for h in range(heads):
        state = state_ref[h]
        deep = jnp.concatenate([grads[h], state.astype(BF16)], axis=0)
        state_ref[h] = through_of(heads, aux, h) * state + mm(mix_ref[0, h, :, 0:dk], deep, TN)


def back_chain_kernel(sizes, mix_ref, grad_ref, aux_ref, end_ref, state_ref):
    heads, dk, dv = sizes

    @pl.when(pl.program_id(0) == 0)
    def _():
        state_ref[...] = end_ref[...]

    grads = [grad_ref[:, h * dv : (h + 1) * dv] for h in range(heads)]
    back_chain_step(sizes, aux_ref[...], mix_ref, grads, state_ref)


def back_chain(sizes, mix, grad, aux, end):
    heads, dk, dv = sizes
    span = grad.shape[0]
    blocks = span // CHUNK
    c = CHUNK
    last = blocks - 1
    rowed = lambda w: pl.BlockSpec((c, w), lambda i: (last - i, 0))
    return pl.pallas_call(
        functools.partial(back_chain_kernel, sizes),
        grid=(blocks,),
        in_specs=[
            pl.BlockSpec((1, heads, c + dk, c + dk), lambda i: (last - i, 0, 0, 0)),
            rowed(heads * dv), rowed(aux.shape[1]),
            pl.BlockSpec((heads, dk, dv), lambda i: (0, 0, 0)),
        ],
        out_specs=pl.BlockSpec((heads, dk, dv), lambda i: (0, 0, 0)),
        out_shape=jax.ShapeDtypeStruct((heads, dk, dv), F32),
        name="delta_back_chain",
    )(mix, grad, aux, end)


def back_kernel(
    sizes, raw_ref, prev_ref, halo_ref, aux_ref, taps_ref, unit_ref, val_ref, inv_ref, wu_ref,
    mix_ref, just_ref, states_ref, grad_ref, end_ref,
    draw_ref, tail_ref, head_ref, dtaps_ref, daux_ref, dbias_ref,
    state_ref, ext_ref, next_ref, zext_ref, dsil_ref,
):
    heads, dk, dv = sizes
    size, width = raw_ref.shape
    step = pl.program_id(0)
    steps = pl.num_programs(0)

    @pl.when(step == 0)
    def _():
        state_ref[...] = end_ref[...]
        next_ref[...] = jnp.zeros_like(next_ref)
        dtaps_ref[...] = jnp.zeros_like(dtaps_ref)
        dbias_ref[...] = jnp.zeros_like(dbias_ref)

    @pl.when(step == steps - 1)
    def _():
        ext_ref[0:8, :] = halo_ref[...].astype(F32)

    @pl.when(step < steps - 1)
    def _():
        ext_ref[0:8, :] = prev_ref[...].astype(F32)[8:, :]

    x = raw_ref[...].astype(F32)
    ext_ref[8 : 8 + size, :] = x
    aux = aux_ref[...]
    taps = taps_ref[...]
    masks = [aux[:, 2 * heads + 2 + m : 2 * heads + 3 + m] for m in range(3)]
    conv = conv_rows(ext_ref, size, taps, masks)
    sig = jax.nn.sigmoid(conv)
    silu = conv * sig
    seg = aux[:, 2 * heads : 2 * heads + 1]
    before = aux[:, 2 * heads + 1 : 2 * heads + 2]
    rows, cols = iotas(size)
    eye = rows == cols
    lanes = lax.broadcasted_iota(jnp.int32, (size, daux_ref.shape[1]), 1)
    is_last = lax.broadcasted_iota(jnp.int32, (size, 1), 0) == size - 1
    daux = jnp.zeros((size, daux_ref.shape[1]), F32)
    for h in range(heads):
        beta = aux[:, h : h + 1]
        decay = aux[:, heads + h : heads + h + 1]
        fading, carried, last_col = fades(decay, seg, before)
        query = unit_ref[:, h * dk : (h + 1) * dk]
        key = unit_ref[:, (heads + h) * dk : (heads + h + 1) * dk]
        value = val_ref[:, h * dv : (h + 1) * dv]
        inv = inv_ref[:, h * size : (h + 1) * size]
        weight = wu_ref[:, h * (dk + dv) : h * (dk + dv) + dk]
        upper = wu_ref[:, h * (dk + dv) + dk : (h + 1) * (dk + dv)]
        just = just_ref[:, h * size : (h + 1) * size].astype(F32)
        state_in = states_ref[0, h]
        dout = grad_ref[:, h * dv : (h + 1) * dv]
        dend = state_ref[h]
        dend_low = dend.astype(BF16)
        deep = jnp.concatenate([dout, dend_low], axis=0)
        both = mm(mix_ref[0, h], deep, TN)
        through = carried[size - 1 :, :]
        state_ref[h] = through * dend + both[:dk]
        dupd = both[dk:]
        update = (upper.astype(F32) - mm(weight, state_in)).astype(BF16)
        dres = mm(inv, dupd, TN)
        dres_low = dres.astype(BF16)
        left = jnp.concatenate([dout, dres_low], axis=0)
        right = jnp.concatenate([update, state_in], axis=0)
        quad = mm(left, right, NT)
        dscore = quad[:size, :size]
        dq_state = quad[:size, size:]
        dlower = jnp.where(rows > cols, -quad[size:, :size], 0.0)
        dk_state = quad[size:, size:]
        dfaded = mm(update, dend_low, NT)
        dqk = fading * dscore
        dkk = jnp.where(rows > cols, beta * fading, 0.0) * dlower
        query32 = query.astype(F32)
        key32 = key.astype(F32)
        score = mix_ref[0, h, 0:size, dk : dk + size].astype(F32)
        sym = dkk + jnp.transpose(dkk)
        pair = mm(jnp.concatenate([dqk, sym], axis=0), key)
        dquery = carried * dq_state + pair[:size]
        dkey = (
            last_col * dfaded
            + mm(dqk, query, TN)
            - (beta * carried) * dk_state
            + pair[size:]
        )
        kx = jnp.sum(key32 * dk_state, axis=1, keepdims=True)
        dcarried = jnp.sum(query32 * dq_state, axis=1, keepdims=True) - beta * kx
        dcarried = dcarried + jnp.where(
            is_last, jnp.sum(state_in.astype(F32) * dend), 0.0
        )
        dbeta = (
            jnp.sum(dlower * just, axis=1, keepdims=True)
            + jnp.sum(dres * value.astype(F32), axis=1, keepdims=True)
            - carried * kx
        )
        flow = dscore * score + dlower * (beta * just)
        kz = jnp.sum(key32 * dfaded, axis=1, keepdims=True) * last_col
        dtotal = jnp.sum(flow, axis=1, keepdims=True) + dcarried * carried - kz
        dtotal = dtotal + jnp.where(is_last, jnp.sum(kz, axis=0, keepdims=True), 0.0)
        dtotal_row = to_row(dtotal, eye) - jnp.sum(flow, axis=0, keepdims=True)
        ddecay = jnp.sum(jnp.where(cols >= rows, dtotal_row, 0.0), axis=1, keepdims=True)
        slope = 2 * heads + FACTS + h
        daux = daux + jnp.where(lanes == h, dbeta * aux[:, slope : slope + 1], 0.0)
        slope = slope + heads
        daux = daux + jnp.where(lanes == heads + h, ddecay * aux[:, slope : slope + 1], 0.0)
        dsil_ref[:, 2 * heads * dk + h * dv : 2 * heads * dk + (h + 1) * dv] = beta * dres
        for first, grad, scale in ((h, dquery, dk ** (-0.5)), (heads + h, dkey, 1.0)):
            part, norm = unit_parts(silu, first * dk, dk)
            unit = part * norm
            grad = grad * scale
            inner = jnp.sum(unit * grad, axis=1, keepdims=True)
            dsil_ref[:, first * dk : (first + 1) * dk] = norm * (grad - unit * inner)
    daux_ref[...] = daux.astype(BF16)
    dbias_ref[0:1, :] += jnp.sum(daux, axis=0, keepdims=True)
    dconv = dsil_ref[...] * (sig * (1.0 + conv * (1.0 - sig)))
    draw = dconv * taps[0:1, :]
    dtaps_ref[0:1, :] += jnp.sum(dconv * x, axis=0, keepdims=True)
    halo = halo_ref[...].astype(F32)
    head = jnp.zeros((8, width), F32)
    for m in (1, 2, 3):
        moved = dconv * masks[m - 1]
        zext_ref[8 : 8 + size, :] = moved
        zext_ref[8 + size :, :] = next_ref[m - 1]
        next_ref[m - 1] = moved[0:8, :]
        shifted = zext_ref[8 + m : 8 + m + size, :]
        draw = draw + shifted * taps[m : m + 1, :]
        dtaps_ref[m : m + 1, :] += jnp.sum(shifted * x, axis=0, keepdims=True)

        @pl.when(step == steps - 1)
        def _():
            zext_ref[0:8, :] = jnp.zeros((8, width), F32)
            edge = zext_ref[m : m + 8, :]
            dtaps_ref[m : m + 1, :] += jnp.sum(edge * halo, axis=0, keepdims=True)
            grown = edge * taps[m : m + 1, :]
            if m == 1:
                head_ref[...] = grown
            else:
                head_ref[...] += grown

    draw_ref[...] = draw.astype(BF16)

    @pl.when(step == 0)
    def _():
        tail_ref[...] = draw[size - 8 :, :]


def back_states(sizes, raw, halo, aux, taps, unit, val, inv, wu, mix, just, states, grad, end):
    heads, dk, dv = sizes
    span, width = raw.shape
    blocks = span // CHUNK
    c = CHUNK
    last = blocks - 1
    rowed = lambda w: pl.BlockSpec((c, w), lambda i: (last - i, 0))
    fixed = lambda shape: pl.BlockSpec(shape, lambda i: (0,) * len(shape))
    per16 = c // 16
    prev = pl.BlockSpec((16, width), lambda i: (jnp.maximum((last - i) * per16 - 1, 0), 0))
    return pl.pallas_call(
        functools.partial(back_kernel, sizes),
        grid=(blocks,),
        in_specs=[
            rowed(width), prev, fixed(halo.shape), rowed(aux.shape[1]), fixed(taps.shape),
            rowed(unit.shape[1]), rowed(val.shape[1]), rowed(inv.shape[1]), rowed(wu.shape[1]),
            pl.BlockSpec((1, heads, c + dk, c + dk), lambda i: (last - i, 0, 0, 0)),
            rowed(just.shape[1]),
            pl.BlockSpec((1, heads, dk, dv), lambda i: (last - i, 0, 0, 0)),
            rowed(heads * dv), fixed(end.shape),
        ],
        out_specs=[
            rowed(width), fixed((8, width)), fixed((8, width)), fixed((8, width)), rowed(128),
            fixed((8, 128)),
        ],
        out_shape=[
            jax.ShapeDtypeStruct((span, width), BF16),
            jax.ShapeDtypeStruct((8, width), F32),
            jax.ShapeDtypeStruct((8, width), F32),
            jax.ShapeDtypeStruct((8, width), F32),
            jax.ShapeDtypeStruct((span, 128), BF16),
            jax.ShapeDtypeStruct((8, 128), F32),
        ],
        scratch_shapes=[
            pltpu.VMEM((heads, dk, dv), F32),
            pltpu.VMEM((c + 8, width), F32),
            pltpu.VMEM((3, 8, width), F32),
            pltpu.VMEM((c + 16, width), F32),
            pltpu.VMEM((c, width), F32),
        ],
        name="delta_back",
    )(raw, raw, halo, aux, taps, unit, val, inv, wu, mix, just, states, grad, end)


MESH = pl.DeviceIdType.MESH
SPAN = 128
PIECES = 2


def line_roles():
    spot = lax.axis_index("tp")
    middle = (spot == 1) | (spot == 2)
    near = jnp.where(spot < 2, 1 - spot, 5 - spot)
    half = jnp.where(spot == 1, 0, 1)
    return middle, near, 3 - spot, half


def enter(grid_peers):
    middle, near, other, _ = line_roles()
    barrier = pltpu.get_barrier_semaphore()
    pl.semaphore_signal(barrier, inc=1, device_id={"tp": near}, device_id_type=MESH)
    waits = 1
    if grid_peers:
        for peer in grid_devices():
            pl.semaphore_signal(barrier, inc=1, device_id=peer, device_id_type=MESH)
            waits += 1

    @pl.when(middle)
    def _():
        pl.semaphore_signal(barrier, inc=1, device_id={"tp": other}, device_id_type=MESH)

    pl.semaphore_wait(barrier, waits + jnp.where(middle, 1, 0))


def grid_devices():
    shard, ctx = lax.axis_index("shard"), lax.axis_index("ctx")
    shards, ctxs = lax.axis_size("shard"), lax.axis_size("ctx")
    peers = []
    for ds in range(shards):
        for dc in range(ctxs):
            if ds or dc:
                peers.append({"shard": (shard + ds) % shards, "ctx": (ctx + dc) % ctxs})
    return peers


class LineSum:
    def __init__(self, count, own, rece, cross, recm, fin, sem):
        self.count = count
        self.own, self.rece, self.cross, self.recm, self.fin = own, rece, cross, recm, fin
        self.sem = sem
        self.middle, self.near, self.other, self.half = line_roles()

    def copy(self, src, dst, kind, piece, device):
        return pltpu.make_async_remote_copy(
            src_ref=src, dst_ref=dst, send_sem=self.sem.at[0, kind, piece],
            recv_sem=self.sem.at[1, kind, piece], device_id={"tp": device}, device_id_type=MESH,
        )

    def up(self, k):
        return self.copy(self.own.at[k], self.rece.at[k], 0, k, self.near)

    def over(self, k):
        return self.copy(self.cross.at[k], self.recm.at[k], 1, k, self.other)

    def final(self, k, kind, half, device):
        place = self.fin.at[k, half]
        return self.copy(place, place, kind, k, device)

    def when(self, k, low, high, what):
        pl.when((k >= low) & (k < high))(what)

    def advance(self, k):
        count = self.count
        mine, theirs = self.half, 1 - self.half

        @pl.when(jnp.logical_not(self.middle) & (k < count))
        def _():
            self.up(k).start()

        @pl.when(self.middle & (k >= 2) & (k < count + 2))
        def _():
            j = k - 2
            self.up(j).wait_recv()
            total = self.own[j, theirs].astype(F32) + self.rece[j, theirs].astype(F32)
            self.cross[j] = total.astype(BF16)
            self.over(j).start()

        @pl.when(self.middle & (k >= 3) & (k < count + 3))
        def _():
            j = k - 3
            self.over(j).wait_recv()
            total = self.own[j, mine].astype(F32) + self.rece[j, mine].astype(F32)
            self.fin[j, mine] = (total + self.recm[j].astype(F32)).astype(BF16)
            self.final(j, 2, mine, self.other).start()
            self.final(j, 3, mine, self.near).start()

        @pl.when(self.middle & (k >= 4) & (k < count + 4))
        def _():
            j = k - 4
            self.final(j, 2, theirs, self.other).wait_recv()
            self.final(j, 4, theirs, self.near).start()

    def arrive(self, k):
        @pl.when(jnp.logical_not(self.middle))
        def _():
            self.final(k, 3, 0, self.near).wait_recv()
            self.final(k, 4, 0, self.near).wait_recv()

    def drain(self):
        def step(k, carry):
            @pl.when(self.middle)
            def _():
                self.over(k).wait_send()
                self.final(k, 2, self.half, self.other).wait_send()
                self.final(k, 3, self.half, self.near).wait_send()
                self.final(k, 4, 1 - self.half, self.near).wait_send()

            @pl.when(jnp.logical_not(self.middle))
            def _():
                self.up(k).wait_send()

            return carry

        lax.fori_loop(0, self.count, step, 0)


def line_scratch(count, rows, width):
    half = rows // 2
    return [
        pltpu.VMEM((count, 2, half, width), BF16),
        pltpu.VMEM((count, 2, half, width), BF16),
        pltpu.VMEM((count, half, width), BF16),
        pltpu.VMEM((count, half, width), BF16),
        pltpu.VMEM((count, 2, half, width), BF16),
        pltpu.SemaphoreType.DMA((2, 5, count)),
    ]


LAG = 3


class ShardSum:
    def __init__(self, parts, axes, bufs, sem):
        self.parts, self.axes, self.bufs, self.sem = parts, axes, bufs, sem
        self.shard, self.ctx = lax.axis_index("shard"), lax.axis_index("ctx")
        self.ctxs = lax.axis_size("ctx")
        self.core, self.row = self.shard % 2, self.shard // 2

    def block(self, item, owner):
        ref, axis = self.parts[item], self.axes[item]
        size = ref.shape[axis] // 4
        cut = pl.ds(pl.multiple_of(owner * size, size), size)
        return ref.at[cut, :] if axis == 0 else ref.at[:, cut]

    def copy(self, src, dst, item, kind, device):
        return pltpu.make_async_remote_copy(
            src_ref=src, dst_ref=dst, send_sem=self.sem.at[0, item, kind],
            recv_sem=self.sem.at[1, item, kind], device_id=device, device_id_type=MESH,
        )

    def swap(self, item, row):
        heard = self.bufs[item][0]
        return self.copy(
            self.block(item, 2 * row + 1 - self.core), heard.at[row], item, row,
            {"shard": 2 * self.row + 1 - self.core},
        )

    def along(self, item):
        _, added, heard, _, _ = self.bufs[item]
        return self.copy(
            added.at[1], heard, item, 2, {"shard": 2 * (1 - self.row) + self.core}
        )

    def across(self, item, distance):
        _, _, _, total, slots = self.bufs[item]
        peer = (self.ctx + distance) % self.ctxs
        return self.copy(total, slots.at[distance], item, 2 + distance, {"ctx": peer})

    def first(self):
        for item in range(len(self.parts)):
            for row in range(2):
                self.swap(item, row).start()

    def second(self, item):
        heard, added, _, _, _ = self.bufs[item]
        for row in range(2):
            self.swap(item, row).wait_recv()
        for place, row in ((1, 1 - self.row), (0, self.row)):
            mine = self.block(item, 2 * row + self.core)[...].astype(F32)
            added[place] = (mine + heard[row].astype(F32)).astype(BF16)
            if place:
                self.along(item).start()

    def third(self, item):
        _, added, heard, total, _ = self.bufs[item]
        self.along(item).wait_recv()
        total[...] = (added[0].astype(F32) + heard[...].astype(F32)).astype(BF16)
        for distance in range(1, self.ctxs):
            self.across(item, distance).start()

    def last(self, item):
        _, _, _, total, slots = self.bufs[item]
        for distance in range(1, self.ctxs):
            self.across(item, distance).wait_recv()
        if self.ctxs == 2:
            return total[...].astype(F32) + slots[1].astype(F32)
        result = None
        for rank in range(self.ctxs):
            gap = (self.ctx - rank) % self.ctxs
            term = jnp.where(
                gap == 0, total[...].astype(F32), slots[jnp.maximum(gap, 1)].astype(F32)
            )
            result = term if result is None else result + term
        return result

    def drain(self, item):
        for row in range(2):
            self.swap(item, row).wait_send()
        self.along(item).wait_send()
        for distance in range(1, self.ctxs):
            self.across(item, distance).wait_send()


def shard_blocks(parts, axes):
    blocks = []
    for part, axis in zip(parts, axes):
        rows, cols = part.shape
        blocks.append((rows // 4, cols) if axis == 0 else (rows, cols // 4))
    return blocks


def shard_scratch(blocks, ctxs):
    bufs = []
    for block in blocks:
        bufs += [
            pltpu.VMEM((2,) + block, BF16), pltpu.VMEM((2,) + block, BF16),
            pltpu.VMEM(block, BF16), pltpu.VMEM(block, BF16),
            pltpu.VMEM((ctxs,) + block, BF16),
        ]
    return bufs + [pltpu.SemaphoreType.DMA((2, len(blocks), 2 + ctxs))]


def pieces_of(total):
    return total.astype(BF16).reshape(PIECES, 2, SPAN // PIECES // 2, total.shape[1])


def normalise(vector):
    rate = lax.rsqrt(jnp.mean(vector * vector, axis=1, keepdims=True) + EPSILON)
    return vector * rate, rate


def norm_back(unit, rate, grad):
    return rate * (grad - unit * jnp.mean(grad * unit, axis=1, keepdims=True))


def out_kernel(
    sizes, blocks, mix_ref, wu_ref, aux_ref, start_ref, gate_ref, gain_ref, weight_ref, tokens_ref,
    gain_two_ref, mixed_ref, states_ref, gated_ref, hidden_ref, normed_ref,
    state_ref, own, rece, cross, recm, fin, sem,
):
    heads, dk, dv = sizes
    line = LineSum(blocks * PIECES, own, rece, cross, recm, fin, sem)
    step = pl.program_id(0)

    @pl.when(step == 0)
    def _():
        state_ref[...] = start_ref[...]
        enter(False)

    @pl.when(step < blocks)
    def _():
        aux = aux_ref[...]
        outs = apply_step(sizes, aux, mix_ref, wu_ref, states_ref, state_ref)
        live = jnp.where(aux[:, 2 * heads : 2 * heads + 1] >= 0.0, 1.0, 0.0)
        parts = []
        for h, out in enumerate(outs):
            cut = slice(h * dv, (h + 1) * dv)
            mixed_ref[:, cut] = out
            unit, _ = normalise(out.astype(F32))
            gate = gate_ref[:, cut]
            gated = unit * gain_ref[:, cut] * (gate * jax.nn.sigmoid(gate)) * live
            parts.append(gated.astype(BF16))
        gated = jnp.concatenate(parts, axis=1)
        gated_ref[...] = gated
        own[pl.ds(step * PIECES, PIECES)] = pieces_of(mm(gated, weight_ref[...]))

    for piece in range(PIECES):
        line.advance(step * PIECES + piece)

    @pl.when(step >= LAG)
    def _():
        for piece in range(PIECES):
            line.arrive((step - LAG) * PIECES + piece)
        attended = fin[pl.ds((step - LAG) * PIECES, PIECES)].reshape(hidden_ref.shape)
        hidden = tokens_ref[...].astype(F32) + attended.astype(F32)
        hidden_ref[...] = hidden
        normed_ref[...] = (normalise(hidden)[0] * gain_two_ref[...]).astype(BF16)

    @pl.when(step == blocks + LAG - 1)
    def _():
        line.drain()


def out_sum(sizes, mix, wu, aux, start, gates, gain, weight, tokens, gain_two):
    heads, dk, dv = sizes
    rows, width = tokens.shape
    blocks = rows // SPAN
    c = SPAN
    early = lambda i: jnp.minimum(i, blocks - 1)
    late = lambda i: jnp.maximum(i - LAG, 0)
    rowed = lambda w: pl.BlockSpec((c, w), lambda i: (early(i), 0))
    after = lambda w: pl.BlockSpec((c, w), lambda i: (late(i), 0))
    fixed = lambda a: pl.BlockSpec(
        a.shape, lambda i: (0,) * a.ndim, pipeline_mode=pl.Buffered(1)
    )
    return pl.pallas_call(
        functools.partial(out_kernel, sizes, blocks),
        grid=(blocks + LAG,),
        in_specs=[
            pl.BlockSpec((1, heads, c + dk, c + dk), lambda i: (early(i), 0, 0, 0)),
            rowed(wu.shape[1]), rowed(aux.shape[1]), fixed(start), rowed(heads * dv),
            fixed(gain), fixed(weight), after(width), fixed(gain_two),
        ],
        out_specs=[
            rowed(heads * dv),
            pl.BlockSpec((1, heads, dk, dv), lambda i: (early(i), 0, 0, 0)),
            rowed(heads * dv), after(width), after(width),
        ],
        out_shape=[
            jax.ShapeDtypeStruct((rows, heads * dv), BF16),
            jax.ShapeDtypeStruct((blocks, heads, dk, dv), BF16),
            jax.ShapeDtypeStruct((rows, heads * dv), BF16),
            jax.ShapeDtypeStruct((rows, width), F32),
            jax.ShapeDtypeStruct((rows, width), BF16),
        ],
        scratch_shapes=[pltpu.VMEM((heads, dk, dv), F32)]
        + line_scratch(blocks * PIECES, SPAN // PIECES, width),
        compiler_params=pltpu.CompilerParams(collective_id=1, has_side_effects=True),
        cost_estimate=pl.CostEstimate(
            flops=4_000_000_000, bytes_accessed=150_000_000, transcendentals=0
        ),
        name="out_sum",
    )(mix, wu, aux, start, gates, gain, weight, tokens, gain_two)


def run_shard_sum(grid_sum, step, outs, starts):
    second, third, last = starts
    for item, (one, two, three) in enumerate(zip(second, third, last)):

        @pl.when(step == one)
        def _():
            grid_sum.second(item)

        @pl.when(step == two)
        def _():
            grid_sum.third(item)

        @pl.when(step == three)
        def _():
            result = grid_sum.last(item)
            first = 0
            for out in outs[item]:
                size = out.shape[1]
                out[...] = result[:, first : first + size]
                first += size
            grid_sum.drain(item)


def mlp_back_kernel(
    sizes, blocks, axes, *refs,
):
    heads, dk, dv = sizes
    items = len(axes)
    (gate_up_a, gate_up_b, weight_a, weight_b, hidden_ref, cot_ref, mixed_ref, gates_ref, aux_ref,
     mix_ref, out_w_ref, gain_ref, gain_two_ref), refs = refs[:13], refs[13:]
    parts, refs = refs[:items], refs[items:]
    (gh_ref, branch_ref, dmixed_ref, dgate_ref, state_ref, dgain_two_ref, dgain_ref), refs = (
        refs[:7], refs[7:],
    )
    outs, refs = refs[:items], refs[items:]
    (own, rece, cross, recm, fin, sem), refs = refs[:6], refs[6:]
    bufs = [refs[5 * i : 5 * i + 5] for i in range(items)]
    grid_sum = ShardSum(parts, axes, bufs, refs[5 * items])
    line = LineSum(blocks * PIECES, own, rece, cross, recm, fin, sem)
    step = pl.program_id(0)

    @pl.when(step == 0)
    def _():
        state_ref[...] = jnp.zeros_like(state_ref)
        dgain_two_ref[...] = jnp.zeros_like(dgain_two_ref)
        dgain_ref[...] = jnp.zeros_like(dgain_ref)
        enter(True)
        grid_sum.first()

    @pl.when(step < blocks)
    def _():
        total = mm(gate_up_a[...], weight_a[...], NT) + mm(gate_up_b[...], weight_b[...], NT)
        own[pl.ds(step * PIECES, PIECES)] = pieces_of(total)

    for piece in range(PIECES):
        line.advance(step * PIECES + piece)
    run_shard_sum(grid_sum, step, [[o] for o in outs], ((1, 1, 2), (4, 6, 8), (10, 10, 10)))

    @pl.when(step >= LAG)
    def _():
        for piece in range(PIECES):
            line.arrive((step - LAG) * PIECES + piece)
        grad = fin[pl.ds((step - LAG) * PIECES, PIECES)].reshape(gh_ref.shape).astype(F32)
        unit, rate = normalise(hidden_ref[...])
        dgain_two_ref[0:1, :] += jnp.sum(grad * unit, axis=0, keepdims=True)
        grad = cot_ref[...].astype(F32) + norm_back(unit, rate, grad * gain_two_ref[...])
        gh_ref[...] = grad
        branch = grad.astype(BF16)
        branch_ref[...] = branch
        aux = aux_ref[...]
        live = jnp.where(aux[:, 2 * heads : 2 * heads + 1] >= 0.0, 1.0, 0.0)
        dgated = mm(branch, out_w_ref[...], NT) * live
        dmixed = []
        for h in range(heads):
            cut = slice(h * dv, (h + 1) * dv)
            unit, rate = normalise(mixed_ref[:, cut].astype(F32))
            gate = gates_ref[:, cut]
            sig = jax.nn.sigmoid(gate)
            gain = gain_ref[:, cut]
            part = dgated[:, cut]
            flow = part * (gate * sig)
            dgain_ref[0:1, cut] += jnp.sum(flow * unit, axis=0, keepdims=True)
            low = norm_back(unit, rate, flow * gain).astype(BF16)
            dmixed_ref[:, cut] = low
            dmixed.append(low)
            slope = sig * (1.0 + gate * (1.0 - sig))
            dgate_ref[:, cut] = (part * (unit * gain) * slope).astype(BF16)
        back_chain_step(sizes, aux, mix_ref, dmixed, state_ref)

    @pl.when(step == blocks + LAG - 1)
    def _():
        line.drain()


def mlp_back_sum(
    sizes, dgate, dup, gate_w, up_w, hidden, cot, mixed, gates, aux, mix, out_w, gain, gain_two,
    parts, axes,
):
    heads, dk, dv = sizes
    rows, width = cot.shape
    blocks = rows // SPAN
    top = blocks - 1
    c = SPAN
    early = lambda i: top - jnp.minimum(i, top)
    late = lambda i: top - jnp.maximum(i - LAG, 0)
    rowed = lambda w: pl.BlockSpec((c, w), lambda i: (early(i), 0))
    after = lambda w: pl.BlockSpec((c, w), lambda i: (late(i), 0))
    whole = lambda shape: pl.BlockSpec(
        shape, lambda i: (0,) * len(shape), pipeline_mode=pl.Buffered(1)
    )
    keep = lambda shape: pl.BlockSpec(shape, lambda i: (0,) * len(shape))
    owned = shard_blocks(parts, axes)
    units = gate_w.shape[1]
    return pl.pallas_call(
        functools.partial(mlp_back_kernel, sizes, blocks, axes),
        grid=(blocks + LAG,),
        in_specs=[
            rowed(units), rowed(units), whole(gate_w.shape), whole(up_w.shape), after(width),
            after(width), after(heads * dv), after(heads * dv), after(aux.shape[1]),
            pl.BlockSpec((1, heads, c + dk, c + dk), lambda i: (late(i), 0, 0, 0)),
            whole(out_w.shape), whole(gain.shape), whole(gain_two.shape),
        ]
        + [whole(p.shape) for p in parts],
        out_specs=[
            after(width), after(width), after(heads * dv), after(heads * dv),
            keep((heads, dk, dv)), keep((8, width)), keep((8, heads * dv)),
        ]
        + [keep(b) for b in owned],
        out_shape=[
            jax.ShapeDtypeStruct((rows, width), F32),
            jax.ShapeDtypeStruct((rows, width), BF16),
            jax.ShapeDtypeStruct((rows, heads * dv), BF16),
            jax.ShapeDtypeStruct((rows, heads * dv), BF16),
            jax.ShapeDtypeStruct((heads, dk, dv), F32),
            jax.ShapeDtypeStruct((8, width), F32),
            jax.ShapeDtypeStruct((8, heads * dv), F32),
        ]
        + [jax.ShapeDtypeStruct(b, F32) for b in owned],
        scratch_shapes=line_scratch(blocks * PIECES, SPAN // PIECES, width)
        + shard_scratch(owned, lax.axis_size("ctx")),
        compiler_params=pltpu.CompilerParams(collective_id=2, has_side_effects=True),
        cost_estimate=pl.CostEstimate(
            flops=6_000_000_000, bytes_accessed=150_000_000, transcendentals=0
        ),
        name="mlp_back_sum",
    )(
        dgate, dup, gate_w, up_w, hidden, cot, mixed, gates, aux, mix, out_w, gain, gain_two,
        *parts,
    )


class TinySum:
    def __init__(self, shares, slots, sem):
        self.shares, self.slots, self.sem = shares, slots, sem
        self.shard, self.ctx = lax.axis_index("shard"), lax.axis_index("ctx")
        self.shards, self.ctxs = lax.axis_size("shard"), lax.axis_size("ctx")

    def copy(self, index, device):
        me = self.shard * self.ctxs + self.ctx
        return pltpu.make_async_remote_copy(
            src_ref=self.shares.at[device["shard"]], dst_ref=self.slots.at[me],
            send_sem=self.sem.at[0, index], recv_sem=self.sem.at[1, index],
            device_id=device, device_id_type=MESH,
        )

    def run(self):
        me = self.shard * self.ctxs + self.ctx
        self.slots[me] = self.shares[self.shard]
        copies = [self.copy(i, device) for i, device in enumerate(grid_devices())]
        for copy in copies:
            copy.start()
        for copy in copies:
            copy.wait()
        total = self.slots[0]
        for index in range(1, self.shards * self.ctxs):
            total = total + self.slots[index]
        return total


def mixer_back_kernel(sizes, blocks, axes, cuts, *refs):
    items = len(axes)
    (draw_ref, dgate_ref, dsmall_ref, weight_ref, tokens_ref, gh_ref, gain_ref, tiny_ref), refs = (
        refs[:8], refs[8:],
    )
    parts, refs = refs[:items], refs[items:]
    (grad_ref, tiny_out), refs = refs[:2], refs[2:]
    outs = []
    for cut in cuts:
        outs.append(refs[:cut])
        refs = refs[cut:]
    (own, rece, cross, recm, fin, sem), refs = refs[:6], refs[6:]
    bufs = [refs[5 * i : 5 * i + 5] for i in range(items)]
    grid_sum = ShardSum(parts, axes, bufs, refs[5 * items])
    dgain_ref, shares, slots, tiny_sem = refs[5 * items + 1 :]
    line = LineSum(blocks * PIECES, own, rece, cross, recm, fin, sem)
    step = pl.program_id(0)
    wide = draw_ref.shape[1]
    gated = dgate_ref.shape[1]

    @pl.when(step == 0)
    def _():
        dgain_ref[...] = jnp.zeros_like(dgain_ref)
        enter(True)
        grid_sum.first()

    @pl.when(step < blocks)
    def _():
        total = mm(draw_ref[...], weight_ref[:, :wide], NT)
        total = total + mm(dgate_ref[...], weight_ref[:, wide : wide + gated], NT)
        total = total + mm(dsmall_ref[...], weight_ref[:, wide + gated :], NT)
        own[pl.ds(step * PIECES, PIECES)] = pieces_of(total)

    for piece in range(PIECES):
        line.advance(step * PIECES + piece)
    run_shard_sum(
        grid_sum, step, outs, ((1, 1, 2, 2), (4, 6, 6, 8), (8, 10, 10, 10))
    )

    @pl.when(step >= LAG)
    def _():
        for piece in range(PIECES):
            line.arrive((step - LAG) * PIECES + piece)
        grad = fin[pl.ds((step - LAG) * PIECES, PIECES)].reshape(grad_ref.shape).astype(F32)
        unit, rate = normalise(tokens_ref[...].astype(F32))
        dgain_ref[0:1, :] += jnp.sum(grad * unit, axis=0, keepdims=True)
        grad_ref[...] = gh_ref[...] + norm_back(unit, rate, grad * gain_ref[...])

    @pl.when(step == blocks + LAG - 1)
    def _():
        shares[...] = tiny_ref[...]
        share = dgain_ref.shape[1] // 4
        for owner in range(4):
            for line_at in range(share // 128):
                first = owner * share + line_at * 128
                shares[owner, line_at : line_at + 1, :] = dgain_ref[0:1, first : first + 128]
        tiny_out[...] = TinySum(shares, slots, tiny_sem).run()
        line.drain()


def mixer_back_sum(sizes, draw, dgate, dsmall, weight, tokens, gh, gain, tiny, parts, axes, splits):
    rows, width = tokens.shape
    blocks = rows // SPAN
    c = SPAN
    early = lambda i: jnp.minimum(i, blocks - 1)
    late = lambda i: jnp.maximum(i - LAG, 0)
    rowed = lambda w: pl.BlockSpec((c, w), lambda i: (early(i), 0))
    after = lambda w: pl.BlockSpec((c, w), lambda i: (late(i), 0))
    whole = lambda shape: pl.BlockSpec(
        shape, lambda i: (0,) * len(shape), pipeline_mode=pl.Buffered(1)
    )
    keep = lambda shape: pl.BlockSpec(shape, lambda i: (0,) * len(shape))
    owned = shard_blocks(parts, axes)
    results = []
    for block, split in zip(owned, splits):
        results += [(block[0], w) for w in split]
    devices = lax.axis_size("shard") * lax.axis_size("ctx")
    return pl.pallas_call(
        functools.partial(mixer_back_kernel, sizes, blocks, axes, [len(s) for s in splits]),
        grid=(blocks + LAG,),
        in_specs=[
            rowed(draw.shape[1]), rowed(dgate.shape[1]), rowed(dsmall.shape[1]),
            whole(weight.shape), after(width), after(width), whole(gain.shape), whole(tiny.shape),
        ]
        + [whole(p.shape) for p in parts],
        out_specs=[after(width), keep(tiny.shape[1:])] + [keep(r) for r in results],
        out_shape=[
            jax.ShapeDtypeStruct((rows, width), F32),
            jax.ShapeDtypeStruct(tiny.shape[1:], F32),
        ]
        + [jax.ShapeDtypeStruct(r, F32) for r in results],
        scratch_shapes=line_scratch(blocks * PIECES, SPAN // PIECES, width)
        + shard_scratch(owned, lax.axis_size("ctx"))
        + [
            pltpu.VMEM((8, width), F32), pltpu.VMEM(tiny.shape, F32),
            pltpu.VMEM((devices,) + tiny.shape[1:], F32),
            pltpu.SemaphoreType.DMA((2, devices - 1)),
        ],
        compiler_params=pltpu.CompilerParams(collective_id=3, has_side_effects=True),
        cost_estimate=pl.CostEstimate(
            flops=6_000_000_000, bytes_accessed=150_000_000, transcendentals=0
        ),
        name="mixer_back_sum",
    )(draw, dgate, dsmall, weight, tokens, gh, gain, tiny, *parts)


def dot_plain(left, right):
    return jnp.dot(left, right, preferred_element_type=F32)


def dot_back(left, right):
    return lax.dot_general(left, right, NT, preferred_element_type=F32)


def dot_outer(left, right):
    return lax.dot_general(left, right, TN, preferred_element_type=F32).astype(BF16)


def row_facts(segment_ids, first, span):
    def at(offset):
        moved = segment_ids
        if offset:
            moved = jnp.concatenate(
                [jnp.full((offset,), -2, jnp.int32), segment_ids[:-offset]], axis=0
            )
        return lax.dynamic_slice_in_dim(moved, first, span)

    here = at(0)
    before = jnp.repeat(at(1).reshape(-1, CHUNK)[:, 0], CHUNK)
    flags = [here == before] + [here == at(m) for m in (1, 2, 3)]
    return jnp.stack([here.astype(F32)] + [f.astype(F32) for f in flags], axis=1)


def shards(
    tokens, segment_ids, cotangent, norm_gain, w_query, w_key, w_value, w_outgate, w_beta, w_decay,
    decay_bias, conv_query, conv_key, conv_value, out_gain, w_out, mlp_gain, w_gate, w_up, w_down,
):
    ctx_size = lax.axis_size("ctx")
    ctx_rank = lax.axis_index("ctx")
    shard_size = lax.axis_size("shard")
    rows_here, model = tokens.shape
    heads = decay_bias.shape[0]
    dk = conv_query.shape[2] * shard_size
    dv = conv_value.shape[2] * shard_size
    sizes = (heads, dk, dv)
    gather = lambda v, axis: lax.all_gather(v, "shard", axis=axis, tiled=True)
    spare = jnp.zeros((w_beta.shape[0], 128 - 2 * heads), BF16)
    mixer_w = gather(
        jnp.concatenate([w_query, w_key, w_value, w_outgate, w_beta, w_decay, spare], axis=1), 0
    )
    tiny = [norm_gain, mlp_gain, conv_query, conv_key, conv_value, out_gain]
    flat = jnp.concatenate([v.reshape(-1) for v in tiny])
    flat = lax.all_gather(flat, "shard", axis=0)
    out_w = gather(w_out, 1)
    gate_w = gather(w_gate, 0)
    up_w = gather(w_up, 0)
    down_w = gather(w_down, 1)
    cuts, at = [], 0
    for v in tiny:
        cuts.append(flat[:, at : at + v.size].reshape((shard_size,) + v.shape))
        at += v.size
    gain_one = cuts[0].reshape(1, -1).astype(F32)
    gain_two = cuts[1].reshape(1, -1).astype(F32)
    taps = [jnp.moveaxis(c, 0, 2).reshape(c.shape[1], -1) for c in cuts[2:5]]
    taps = jnp.concatenate(taps, axis=1).astype(F32)
    head_gain = jnp.moveaxis(cuts[5], 0, 1).reshape(1, heads * dv).astype(F32)
    conv_width = taps.shape[1]
    facts = row_facts(segment_ids, ctx_rank * rows_here, rows_here)
    bias = jnp.zeros((1, 128), F32)
    bias = lax.dynamic_update_slice(bias, decay_bias.astype(F32)[None], (0, heads))

    inputs32 = tokens.astype(F32)
    normed = (normalise(inputs32)[0] * gain_one).astype(BF16)
    raw = dot_plain(normed, mixer_w[:, :conv_width]).astype(BF16)
    gates = dot_plain(normed, mixer_w[:, conv_width:])
    ahead = [(i, i + 1) for i in range(ctx_size - 1)]
    behind = [(i + 1, i) for i in range(ctx_size - 1)]
    halo = lax.ppermute(raw[rows_here - 8 :], "ctx", ahead)
    unit, val, inv, wu, mix, just, total, aux = prepare(
        sizes, raw, halo, gates, bias, facts, taps
    )
    start = lax.ppermute(total, "ctx", ahead)
    for _ in range(ctx_size - 2):
        start = lax.ppermute(apply_states(sizes, mix, wu, aux, start)[2], "ctx", ahead)
    mixed, states, gated, hidden_in, normed_two = out_sum(
        sizes, mix, wu, aux, start, gates, head_gain, out_w, tokens, gain_two
    )

    gate_two = dot_plain(normed_two, gate_w)
    up_two = dot_plain(normed_two, up_w)
    sigmoid_two = jax.nn.sigmoid(gate_two)
    activated = gate_two * sigmoid_two
    hidden = (activated * up_two).astype(BF16)
    grad_hidden = dot_back(cotangent, down_w)
    gate_slope = sigmoid_two * (1.0 + gate_two * (1.0 - sigmoid_two))
    grad_gate = (grad_hidden * up_two * gate_slope).astype(BF16)
    grad_up = (grad_hidden * activated).astype(BF16)
    mlp_part = dot_plain(hidden, down_w).astype(BF16)
    mlp_parts = [
        dot_outer(normed_two, grad_gate),
        dot_outer(normed_two, grad_up),
        dot_outer(hidden, cotangent),
    ]
    found = mlp_back_sum(
        sizes, grad_gate, grad_up, gate_w, up_w, hidden_in, cotangent, mixed, gates, aux, mix,
        out_w, head_gain, gain_two, mlp_parts, (0, 0, 1),
    )
    gh, branch, grad_mixed, grad_gate_low, chain, grad_gain_two, grad_head_gain = found[:7]
    part_gate, part_up, part_down = found[7:]
    mlp_part, gh = lax.optimization_barrier((mlp_part, gh))
    mlp_out = lax.psum(mlp_part, "tp")
    result = (hidden_in + mlp_out.astype(F32)).astype(BF16)
    end = lax.ppermute(chain, "ctx", behind)
    for _ in range(ctx_size - 2):
        end = lax.ppermute(back_chain(sizes, mix, grad_mixed, aux, end), "ctx", behind)
    draw, tail, head, dtaps, dsmall, dbias = back_states(
        sizes, raw, halo, aux, taps, unit, val, inv, wu, mix, just, states, grad_mixed, end
    )
    tail = (tail + lax.ppermute(head, "ctx", behind)).astype(BF16)
    draw = lax.dynamic_update_slice(draw, tail, (rows_here - 8, 0))
    taps_parts = []
    first = 0
    for width in (heads * dk, heads * dk, heads * dv):
        part = dtaps[:4, first : first + width].reshape(4, heads, shard_size, -1)
        taps_parts.append(jnp.moveaxis(part, 2, 0))
        first += width
    lines = lambda v: v.reshape(shard_size, -1, 128)
    bias_row = jnp.broadcast_to(dbias[0:1][None], (shard_size, 1, 128))
    tiny_grads = [
        jnp.zeros((shard_size, norm_gain.shape[0] // 128, 128), F32), lines(grad_gain_two[0]),
        bias_row, *[lines(p) for p in taps_parts],
        lines(jnp.moveaxis(grad_head_gain[0].reshape(heads, shard_size, -1), 1, 0)),
    ]
    tiny_grads = jnp.concatenate(tiny_grads, axis=1)
    tiny_grads = jnp.pad(tiny_grads, ((0, 0), (0, -tiny_grads.shape[1] % 8), (0, 0)))
    mixer_parts = [
        dot_outer(normed, draw), dot_outer(normed, grad_gate_low), dot_outer(normed, dsmall),
        dot_outer(gated, branch),
    ]
    qw, vw = heads * dk, heads * dv
    found = mixer_back_sum(
        sizes, draw, grad_gate_low, dsmall, mixer_w, tokens, gh, gain_one, tiny_grads,
        mixer_parts, (0, 0, 0, 1),
        ((qw, qw, vw), (vw,), (128,), (model // shard_size,)),
    )
    input_grad, mine, part_query, part_key, part_value, part_outgate, part_small, part_out = found
    shapes = [
        norm_gain.shape, mlp_gain.shape, (128,), conv_query.shape, conv_key.shape,
        conv_value.shape, out_gain.shape,
    ]
    small, at = [], 0
    for shape in shapes:
        count = 1
        for n in shape:
            count *= n
        small.append(mine[at : at + count // 128].reshape(shape))
        at += count // 128
    return (
        result,
        input_grad,
        small[0],
        part_query,
        part_key,
        part_value,
        part_outgate,
        part_small[:, :heads],
        part_small[:, heads : 2 * heads],
        small[2][heads : 2 * heads],
        small[3],
        small[4],
        small[5],
        small[6],
        part_out,
        small[1],
        part_gate,
        part_up,
        part_down,
    )


def solution(mesh):
    rows = P(("shard", "ctx"), None)
    cols = P("shard", "tp")
    taps = P(None, "tp", "shard")
    turned = P("tp", "shard")
    in_specs = (
        rows, P("shard"), rows, P("shard"), cols, cols, cols, cols, cols, cols, P("tp"),
        taps, taps, taps, turned, turned, P("shard"), cols, cols, turned,
    )
    out_specs = (
        rows, rows, P("shard"), cols, cols, cols, cols, cols, cols, P("tp"),
        taps, taps, taps, turned, turned, P("shard"), cols, cols, turned,
    )
    return jax.shard_map(shards, mesh=mesh, in_specs=in_specs, out_specs=out_specs, check_vma=False)
```
